32 devices in a mesh: leaf: 8 (over z, y), front: 4 (over x, core).
Axes of the slice: x: 2, y: 2, z: 4, core: 2. Of those that a mesh axis runs over, the one named last changes fastest.
Arguments:
- right_side: float32 [8, 4, 96, 512], P('leaf', 'front'), may hold values from -6 to 6
- factor_inverse: float32 [8, 4, 128, 7680], P('leaf', 'front'), may hold values from -1 to 1, as said below
- update_panel: float32 [8, 4, 128, 1792], P('leaf', 'front'), may hold values from -0.09375 to 0.09375
- update_targets: int32 [8, 14], P('leaf'), may hold values from 0 to 31, as said below
- pivot_pairs: int32 [8, 4, 256], P('leaf', 'front'), may hold values 0 or 1
- pivot_diagonal: float32 [8, 4, 512], P('leaf', 'front'), may hold values from 0.5 to 2
- pivot_coupling: float32 [8, 4, 256], P('leaf', 'front'), may hold values from 3 to 5
Outputs:
- solution: float32 [8, 4, 96, 512], P('leaf', 'front')
The draws below stay inside these ranges and needn't reach their ends.
Inputs may be any that keep to these rules, and one draw needn't show every extreme that they name: `factor_inverse`: each front's inverse factor is lower triangular in the front's row order with ones on its diagonal. `update_targets`: each front's list names distinct blocks of its parent's pivot rows in rising order, and is repeated in the row of every leaf index of the front's group.
All inputs are finite; a program needn't handle non-finite values. No bound on the sum of `pivot_pairs` on one device may be relied on, other than what follows from the above.
Results may differ from the reference program's by a relative error of at most 0.0001.
Values sent between devices are 32-bit elements; how exact they have to be, the bound alone decides.
A program may use at most 64 MiB of HBM per device.

```python
import math
import jax
import jax.numpy as jnp
from jax import lax

PB = 128
R = 96
LEVELS = 4
BLOCK = 128
UCOLS = 1792
N_LEAF = 8
N_FRONT = 4


def draw_factor_inverse(key, part):
    leaf_ids = jnp.arange(N_LEAF, dtype=jnp.int32)[:, None, None, None]
    front_ids = jnp.arange(N_FRONT, dtype=jnp.int32)[None, :, None, None]
    row_ids = jnp.arange(PB, dtype=jnp.int32)[None, None, :, None]
    pieces = []
    for level_index in range(LEVELS):
        group_width = 2 ** level_index
        front_span = N_FRONT * PB * group_width
        column = jnp.arange(front_span, dtype=jnp.int32)[None, None, None, :]
        row_order = (front_ids * group_width + leaf_ids % group_width) * PB + row_ids
        level_key = jax.random.fold_in(key, 11 + level_index)
        shape_all = (N_LEAF, N_FRONT, PB, front_span)
        noise_part = jax.random.normal(level_key, shape_all, jnp.float32)
        noise_part = noise_part * (0.5 / math.sqrt(front_span))
        level_block = jnp.where(column < row_order, noise_part, 0.0) + jnp.where(column == row_order, 1.0, 0.0)
        pieces.append(level_block.astype(jnp.float32))
    return jnp.concatenate(pieces, axis=-1)


def draw_update_targets(key, part):
    target_lists = []
    for level_index in range(LEVELS - 1):
        group_width = 2 ** level_index
        node_count = N_LEAF // group_width
        block_count = 2 * PB * group_width // BLOCK
        parent_blocks = N_FRONT * PB * 2 * group_width // BLOCK
        scores = jax.random.randint(jax.random.fold_in(key, 31 + level_index), (node_count, parent_blocks), 0, 1 << 20)
        scores = scores * parent_blocks + jnp.arange(parent_blocks, dtype=jnp.int32)[None, :]
        node_ids = jnp.arange(node_count, dtype=jnp.int32)[:, None]
        block_ids = jnp.arange(parent_blocks, dtype=jnp.int32)[None, :]
        forced = (node_ids == 0) & (block_ids == parent_blocks - 1) | (node_ids == node_count - 1) & (block_ids == 0)
        scores = jnp.where(forced, -1, scores)
        chosen = jnp.sort(jnp.argsort(scores, axis=1)[:, :block_count].astype(jnp.int32), axis=1)
        target_lists.append(jnp.repeat(chosen, group_width, axis=0))
    return jnp.concatenate(target_lists, axis=1)


def touch_ends(entries, stream_key, least, high):
    dims = entries.shape
    index_at = [jax.random.randint(jax.random.fold_in(stream_key, axis), (), 0, dims[axis]) for axis in range(len(dims))]
    entries = entries.at[tuple(index_at)].set(least)
    longest = dims.index(max(dims))
    index_at[longest] = (index_at[longest] + 1) % dims[longest]
    return entries.at[tuple(index_at)].set(high)


def block_levels(stream_key, extent, split, least, high):
    def one(position, parts):
        heights = jax.random.uniform(jax.random.fold_in(jax.random.fold_in(stream_key, 6), position), (parts,), jnp.float32, least / len(split), high / len(split))
        return jnp.repeat(jnp.exp(heights), extent[position] // parts).reshape((-1,) + (1,) * (len(extent) - position - 1))

    factor_of = one(*split[0])
    for cut in split[1:]:
        factor_of = factor_of * one(*cut)
    return factor_of


def noise(key, dims, deviation, most, shards=(), kind=jnp.bfloat16):
    values = deviation * jax.random.normal(key, dims, jnp.float32)
    if shards:
        values = values * block_levels(key, dims, shards, -0.22, 0.18)
    return jnp.clip(values, -most, most).astype(kind)


def setup_inputs(seed: int = 0) -> dict:
    keys = jax.random.split(jax.random.key(seed), 8)
    right_side = noise(keys[0], (N_LEAF, N_FRONT, R, LEVELS * PB), 1.0, 6.0, ((0, 8), (1, 4)), jnp.float32)
    factor_inverse = draw_factor_inverse(jax.random.fold_in(keys[7], 71), 0)
    update_panel = noise(keys[2], (N_LEAF, N_FRONT, PB, UCOLS), (N_FRONT * PB * 2 ** (LEVELS - 1)) ** -0.5, 0.09375, ((0, 8), (1, 4)), jnp.float32)
    update_targets = draw_update_targets(jax.random.fold_in(keys[7], 71), 0)
    pivot_pairs = touch_ends((jax.random.randint(keys[4], (N_LEAF, N_FRONT, LEVELS * PB // 2), 0, 2) < 1).astype(jnp.int32), jax.random.fold_in(keys[4], 1), 0, 1)
    pivot_diagonal = jnp.clip(jnp.exp(math.log(2.0) - 1.3862944 * jax.random.uniform(keys[5], (N_LEAF, N_FRONT, LEVELS * PB), jnp.float32) ** block_levels(keys[5], (N_LEAF, N_FRONT, LEVELS * PB), ((0, 8), (1, 4)), -0.2, 0.2)), 0.5, 2.0)
    pivot_coupling = jnp.clip(3.0 + 2.0 * jax.random.uniform(keys[6], (N_LEAF, N_FRONT, LEVELS * PB // 2), jnp.float32) ** block_levels(keys[6], (N_LEAF, N_FRONT, LEVELS * PB // 2), ((0, 8), (1, 4)), -0.2, 0.2), 3.0, 5.0)
    return dict(right_side=right_side, factor_inverse=factor_inverse, update_panel=update_panel, update_targets=update_targets, pivot_pairs=pivot_pairs, pivot_diagonal=pivot_diagonal, pivot_coupling=pivot_coupling)


exact_mode = lax.Precision.HIGHEST


def front_of(values, level_index):
    group_width = 2 ** level_index
    node_count = N_LEAF // group_width
    side_count = values.shape[2]
    shaped = values.reshape(node_count, group_width, N_FRONT, side_count, PB)
    return shaped.transpose(0, 3, 2, 1, 4).reshape(node_count, side_count, N_FRONT * group_width * PB)


def spread_rows(front_values, level_index):
    group_width = 2 ** level_index
    node_count = N_LEAF // group_width
    side_count = front_values.shape[1]
    shaped = front_values.reshape(node_count, side_count, N_FRONT, group_width, PB)
    return shaped.transpose(0, 3, 2, 1, 4).reshape(N_LEAF, N_FRONT, side_count, PB)


def pivot_solve(solved, pivot_diag, couple, pivot_kinds):
    pair_first = solved[..., 0::2]
    second = solved[..., 1::2]
    diag_first = pivot_diag[..., 0::2][:, :, None, :]
    diag_second = pivot_diag[..., 1::2][:, :, None, :]
    coupling = couple[:, :, None, :]
    pair_flag = (pivot_kinds == 1)[:, :, None, :]
    determinant = diag_first * diag_second - coupling * coupling
    two_first = (diag_second * pair_first - coupling * second) / determinant
    two_second = (diag_first * second - coupling * pair_first) / determinant
    result_first = jnp.where(pair_flag, two_first, pair_first / diag_first)
    result_second = jnp.where(pair_flag, two_second, second / diag_second)
    return jnp.stack([result_first, result_second], axis=-1).reshape(solved.shape)


def target_table(update_targets, level_index):
    group_width = 2 ** level_index
    block_count = 2 * PB * group_width // BLOCK
    target_start = 2 * PB * (group_width - 1) // BLOCK
    parent_blocks = N_FRONT * PB * 2 * group_width // BLOCK
    target_lists = update_targets[::group_width, target_start:target_start + block_count]
    ids = jnp.arange(parent_blocks, dtype=jnp.int32)
    return (target_lists[:, :, None] == ids[None, None, :]).astype(jnp.float32)


def reference(right_side, factor_inverse, update_panel, update_targets, pivot_pairs, pivot_diagonal, pivot_coupling):
    side_count = right_side.shape[2]
    carried = jnp.zeros((N_LEAF, N_FRONT, side_count, PB), jnp.float32)
    weighted = []
    half_pb = PB // 2
    for level_index in range(LEVELS):
        group_width = 2 ** level_index
        node_count = N_LEAF // group_width
        front_span = N_FRONT * PB * group_width
        column_start = N_FRONT * PB * (group_width - 1)
        inverse_rows = factor_inverse[..., column_start:column_start + front_span]
        own_side = right_side[..., level_index * PB:(level_index + 1) * PB] - carried
        gathered = jnp.repeat(front_of(own_side, level_index), group_width, axis=0)
        solved = jnp.einsum("dqpc,drc->dqrp", inverse_rows, gathered, precision=exact_mode)
        weighted.append(pivot_solve(solved,
                                    pivot_diagonal[..., level_index * PB:(level_index + 1) * PB],
                                    pivot_coupling[..., level_index * half_pb:(level_index + 1) * half_pb],
                                    pivot_pairs[..., level_index * half_pb:(level_index + 1) * half_pb]))
        if level_index + 1 < LEVELS:
            update_len = 2 * PB * group_width
            update_start = 2 * PB * (group_width - 1)
            update_part = jnp.einsum("dqrp,dqpu->dqru", solved,
                                     update_panel[..., update_start:update_start + update_len], precision=exact_mode)
            summed = update_part.reshape(node_count, group_width, N_FRONT, side_count, update_len).sum(axis=(1, 2))
            onehot_table = target_table(update_targets, level_index)
            placed = jnp.einsum("nrkc,nkt->nrtc", summed.reshape(node_count, side_count, update_len // BLOCK, BLOCK),
                                onehot_table, precision=exact_mode)
            placed = placed.reshape(node_count // 2, 2, side_count, 2 * front_span).sum(axis=1)
            carried = spread_rows(placed, level_index + 1)
    answers = [None] * LEVELS
    for level_index in reversed(range(LEVELS)):
        group_width = 2 ** level_index
        node_count = N_LEAF // group_width
        front_span = N_FRONT * PB * group_width
        column_start = N_FRONT * PB * (group_width - 1)
        inverse_rows = factor_inverse[..., column_start:column_start + front_span]
        target = weighted[level_index]
        if level_index + 1 < LEVELS:
            update_len = 2 * PB * group_width
            update_start = 2 * PB * (group_width - 1)
            parent = jnp.repeat(front_of(answers[level_index + 1], level_index + 1), 2, axis=0)
            onehot_table = target_table(update_targets, level_index)
            chosen = jnp.einsum("nrtc,nkt->nrkc", parent.reshape(node_count, side_count, -1, BLOCK),
                                onehot_table, precision=exact_mode).reshape(node_count, side_count, update_len)
            chosen = jnp.repeat(chosen, group_width, axis=0)
            target = target - jnp.einsum("dru,dqpu->dqrp", chosen,
                                         update_panel[..., update_start:update_start + update_len], precision=exact_mode)
        partial_terms = jnp.einsum("dqrp,dqpc->dqrc", target, inverse_rows, precision=exact_mode)
        summed = partial_terms.reshape(node_count, group_width, N_FRONT, side_count, front_span).sum(axis=(1, 2))
        answers[level_index] = spread_rows(summed, level_index)
    return jnp.concatenate(answers, axis=-1)
```

```python
import functools

import jax
import jax.numpy as jnp
from jax import lax
from jax.experimental import pallas as pl
from jax.experimental.pallas import tpu as pltpu
from jax.sharding import PartitionSpec as P

LEVELS = 4
BLOCK = 128
MESH = pl.DeviceIdType.MESH
F32 = jnp.float32
BF16 = jnp.bfloat16
PRE_FROM = 1
RELAY_FROM = 1
SHARE = 4


def flip(value, mask):
    result = value
    bit = 0
    while mask >> bit:
        if mask >> bit & 1:
            unit = 1 << bit
            result = result + (1 - 2 * lax.rem(lax.div(value, unit), 2)) * unit
        bit += 1
    return result


def split(values):
    high = values.astype(BF16)
    return high, (values - high.astype(F32)).astype(BF16)


def rows_of(values):
    high, low = split(values)
    return jnp.concatenate([high, low], 0)


def square_of(values):
    high, low = split(values)
    return jnp.concatenate(
        [jnp.concatenate([high, high], 1), jnp.concatenate([low, low], 1)], 0
    )


def along_columns(stacked, matrix):
    return lax.dot_general(
        stacked, matrix, (((1,), (1,)), ((), ())), preferred_element_type=F32
    )


def fold(product, sides, width):
    return (product[:sides, :width] + product[sides:, :width]) + (
        product[:sides, width:] + product[sides:, width:]
    )


def across(square, matrix, sides):
    product = jnp.dot(square, matrix, preferred_element_type=F32)
    return product[:sides] + product[sides:]


class Plan:
    def __init__(self, fronts, sides):
        self.fronts, self.sides = fronts, sides
        half = sides // 2
        self.gathers = {}
        self.scatters = {}
        for level in range(LEVELS):
            self.gathers["rhs", level] = (level, sides)
            self.scatters["out", level] = (level, sides)
        for level in range(LEVELS - 1):
            self.scatters["up", level] = (level, half)
            self.gathers["up", level] = (level + 1, half)
            self.scatters["down", level] = (level + 1, half)
            self.gathers["down", level] = (level, half)

    def size(self, level):
        return self.fronts << level

    def pre(self, key):
        return self.scatters[key][0] >= (1 if key[0] == "out" else PRE_FROM)

    def relay(self, key):
        return self.gathers[key][0] >= (1 if key[0] == "rhs" else RELAY_FROM)


def kernel(plan, pivots, *refs):
    (
        rhs_ref,
        inverse_hbm,
        update_hbm,
        lists_ref,
        pairs_ref,
        diagonal_ref,
        coupling_ref,
        out_ref,
        inverse_raw,
        update_raw,
        inverse_split,
        update_split,
        targets_ref,
        targets_far,
        targets_smem,
        load_sem,
        targets_send,
        targets_recv,
        gather_send,
        gather_recv,
        scatter_send,
        scatter_recv,
        rhs_send,
        rhs_recv,
        side_send,
        side_recv,
        cross_part,
        cross_first,
        cross_landed,
        cross_row,
        cross_col,
        cross_row_split,
        cross_col_split,
        low_part,
        low_first,
        low_landed,
        low_split,
        *buffers,
    ) = refs
    sides, fronts = plan.sides, plan.fronts
    half = sides // 2
    nx = fronts // 2
    leaf = lax.axis_index("leaf")
    front = lax.axis_index("front")
    core, column = lax.rem(front, 2), lax.div(front, 2)

    gather_keys = list(plan.gathers)
    scatter_keys = list(plan.scatters)
    gather_buffer, part, landed, first = {}, {}, {}, {}
    buffers = list(buffers)
    for key in gather_keys:
        gather_buffer[key] = buffers.pop(0)
    for key in scatter_keys:
        part[key] = buffers.pop(0)
        landed[key] = buffers.pop(0)
        if plan.pre(key):
            first[key] = buffers.pop(0)

    def rank(level):
        return core * (nx << level) + column * (1 << level) + lax.rem(leaf, 1 << level)

    def peer(level, mask):
        return (
            flip(leaf, mask % (1 << level)),
            flip(column, (mask >> level) % nx) * 2 + flip(core, mask // (nx << level)),
        )

    def slot_block(level, slot):
        slot_core, rest = divmod(slot, nx << level)
        slot_column, offset = divmod(rest, 1 << level)
        return ((slot_column * 2 + slot_core) << level) + offset

    def slot_of(level, block):
        index, part_of = divmod(block, 2)
        return part_of * (nx << level) + index

    def rhs_slot(level):
        if not level:
            return rank(0)
        inside = lax.rem(leaf, 1 << level)
        if level == LEVELS - 1:
            depth = 1 << level - 1
            run = (core * 2 + lax.rem(inside, 2)) * nx + column
            return run * depth + lax.div(inside, 2)
        return (
            core * (nx << level) + lax.div(inside, 2) * (2 * nx) + column * 2 + lax.rem(inside, 2)
        )

    def rhs_block(level, slot):
        if not level:
            return slot_block(0, slot)
        slot_core, rest = divmod(slot, nx << level)
        if level == LEVELS - 1:
            rest, deep = divmod(rest, 1 << level - 1)
            row, slot_column = divmod(rest, nx)
            return ((slot_column * 2 + slot_core) << level) + deep * 2 + row
        deep, rest = divmod(rest, 2 * nx)
        slot_column, row = divmod(rest, 2)
        return ((slot_column * 2 + slot_core) << level) + deep * 2 + row

    sends = []

    def send(source, target, send_sem, recv_sem, device):
        pltpu.make_async_remote_copy(
            source, target, send_sem, recv_sem, device_id=device, device_id_type=MESH
        ).start()

    def wait_recv(buffer, count, send_sem, recv_sem):
        span = buffer.at[pl.ds(0, count)]
        pltpu.make_async_remote_copy(
            span, span, send_sem, recv_sem, device_id=peer(0, 1), device_id_type=MESH
        ).wait_recv()

    def wait_send(buffer, count, send_sem, recv_sem):
        span = buffer.at[pl.ds(0, count)]
        pltpu.make_async_remote_copy(
            span, span, send_sem, recv_sem, device_id=peer(0, 1), device_id_type=MESH
        ).wait_send()

    bulk = []

    def issue(count):
        for _ in range(min(count, len(bulk))):
            bulk.pop(0)()

    def far_first(count):
        return sorted(range(1, count), key=lambda mask: -bin(mask).count("1"))

    def gather_start(key, later=False):
        level, _ = plan.gathers[key]
        buffer, index = gather_buffer[key], gather_keys.index(key)
        mine = rank(level)
        sems = gather_send.at[index, 0], gather_recv.at[index, 0]
        count = nx << level if plan.relay(key) else fronts << level
        for mask in far_first(count):

            def one(mask=mask):
                send(buffer.at[mine], buffer.at[mine], *sems, peer(level, mask))

            bulk.append(one) if later else one()
        sends.append((buffer, count - 1, *sems))

    def gather_forward(key):
        level, _ = plan.gathers[key]
        buffer, index = gather_buffer[key], gather_keys.index(key)
        count = nx << level
        if not plan.relay(key):
            return
        wait_recv(buffer, count - 1, gather_send.at[index, 0], gather_recv.at[index, 0])
        span = buffer.at[pl.ds(core * count, count)]
        sems = gather_send.at[index, 1], gather_recv.at[index, 1]
        send(span, span, *sems, peer(level, count))
        sends.append((buffer, count, *sems))

    def gather_finish(key):
        level, _ = plan.gathers[key]
        index = gather_keys.index(key)
        step = 1 if plan.relay(key) else 0
        count = nx << level if step else (fronts << level) - 1
        wait_recv(
            gather_buffer[key], count, gather_send.at[index, step], gather_recv.at[index, step]
        )

    def rhs_sems(level, phase):
        return rhs_send.at[level, phase], rhs_recv.at[level, phase]

    def for_column(body):
        for index in range(nx):

            @pl.when(column == index)
            def _():
                body(index)

    def rhs_across(level):
        @pl.when(column == 0)
        def _():
            slot = gather_buffer["rhs", level].at[rhs_slot(level)]
            send(slot, slot, *rhs_sems(level, 0), peer(level, 1 << level))

    def rhs_beside(level):
        buffer = gather_buffer["rhs", level]

        def body(index):
            if index:
                wait_recv(buffer, index, *rhs_sems(level, 0))
            for back in range(index + 1):
                slot = buffer.at[rhs_slot(level) - 2 * back]
                send(slot, slot, *rhs_sems(level, 1), peer(level, 1))

        for_column(body)

    def rhs_deep(level):
        buffer, depth = gather_buffer["rhs", level], 1 << level - 1
        start = core * (nx << level) + lax.div(lax.rem(leaf, 1 << level), 2) * (2 * nx)

        def body(index):
            wait_recv(buffer, index + 1, *rhs_sems(level, 1))
            span = buffer.at[pl.ds(start, 2 * (index + 1))]
            for deep in range(1, depth):
                send(span, span, *rhs_sems(level, 2), peer(level, 2 * deep))

        for_column(body)

    top = LEVELS - 1
    top_depth = 1 << top - 1

    def top_run(row, slot_column):
        start = ((core * 2 + row) * nx + slot_column) * top_depth
        return gather_buffer["rhs", top].at[pl.ds(start, top_depth)]

    def top_deep():
        slot = gather_buffer["rhs", top].at[rhs_slot(top)]
        for deep in range(top_depth - 1, 0, -1):
            send(slot, slot, *rhs_sems(top, 0), peer(top, 2 * deep))
        sends.append((gather_buffer["rhs", top], top_depth - 1, *rhs_sems(top, 0)))

    def top_first():
        row = lax.rem(leaf, 2)
        wait_recv(gather_buffer["rhs", top], top_depth - 1, *rhs_sems(top, 0))
        run = top_run(row, column)
        send(run, run, *rhs_sems(top, 2), peer(top, 1))
        sends.append((gather_buffer["rhs", top], top_depth, *rhs_sems(top, 2)))

        @pl.when((column == 0) & (core == 0))
        def _():
            span = top_run(row, 0)
            send(span, span, *rhs_sems(top, 1), peer(top, 1 << top))

    def top_second():
        row = lax.rem(leaf, 2)
        buffer = gather_buffer["rhs", top]

        @pl.when((column == 0) & (core == 1))
        def _():
            wait_recv(buffer, top_depth, *rhs_sems(top, 2))
            for each in range(2):
                span = top_run(each, 0)
                send(span, span, *rhs_sems(top, 1), peer(top, 1 << top))

        @pl.when((column == 1) & (core == 0))
        def _():
            wait_recv(buffer, top_depth, *rhs_sems(top, 1))
            span = top_run(row, 0)
            send(span, span, *rhs_sems(top, 2), peer(top, 1))

    def top_relay():
        buffer = gather_buffer["rhs", top]

        @pl.when((column == 0) & (core == 0))
        def _():
            wait_recv(buffer, top_depth, *rhs_sems(top, 2))

        @pl.when((column == 1) & (core == 0))
        def _():
            wait_recv(buffer, 2 * top_depth, *rhs_sems(top, 2))

        @pl.when((column == 1) & (core == 1))
        def _():
            wait_recv(buffer, top_depth, *rhs_sems(top, 2))
            wait_recv(buffer, 2 * top_depth, *rhs_sems(top, 1))

        span = buffer.at[pl.ds(core * (nx << top), nx << top)]
        send(span, span, *rhs_sems(top, 3), peer(top, nx << top))
        sends.append((buffer, nx << top, *rhs_sems(top, 3)))

    def top_drain():
        buffer = gather_buffer["rhs", top]

        @pl.when((column == 0) & (core == 0))
        def _():
            wait_send(buffer, top_depth, *rhs_sems(top, 1))

        @pl.when((column == 0) & (core == 1))
        def _():
            wait_send(buffer, 2 * top_depth, *rhs_sems(top, 1))

        @pl.when((column == 1) & (core == 0))
        def _():
            wait_send(buffer, top_depth, *rhs_sems(top, 2))

    def rhs_relay(level):
        buffer, depth = gather_buffer["rhs", level], 1 << level - 1

        def body(index):
            if depth > 1:
                wait_recv(buffer, 2 * (depth - 1) * (index + 1), *rhs_sems(level, 2))
            else:
                wait_recv(buffer, index + 1, *rhs_sems(level, 1))

        for_column(body)
        span = buffer.at[pl.ds(core * (nx << level), nx << level)]
        send(span, span, *rhs_sems(level, 3), peer(level, nx << level))
        sends.append((buffer, nx << level, *rhs_sems(level, 3)))

    def rhs_finish(level):
        wait_recv(gather_buffer["rhs", level], nx << level, *rhs_sems(level, 3))

    def rhs_drain(level):
        buffer, depth = gather_buffer["rhs", level], 1 << level - 1

        def body(index):
            if not index:
                wait_send(buffer, 1, *rhs_sems(level, 0))
            wait_send(buffer, index + 1, *rhs_sems(level, 1))
            if depth > 1:
                wait_send(buffer, 2 * (depth - 1) * (index + 1), *rhs_sems(level, 2))

        for_column(body)

    def scatter_start(key):
        level, _ = plan.scatters[key]
        index = scatter_keys.index(key)
        count = nx << level
        if plan.pre(key):
            sems = scatter_send.at[index, 0], scatter_recv.at[index, 0]
            send(
                part[key].at[pl.ds((1 - core) * count, count)], first[key], *sems, peer(level, count)
            )
            sends.append((part[key], count, *sems))
        else:
            scatter_spread(key, 2 * count)

    def scatter_spread(key, count, later=False):
        level, _ = plan.scatters[key]
        index = scatter_keys.index(key)
        mine = rank(level)
        sems = scatter_send.at[index, 1], scatter_recv.at[index, 1]
        for mask in far_first(count):

            def one(mask=mask):
                send(
                    part[key].at[flip(mine, mask)],
                    landed[key].at[mask - 1],
                    *sems,
                    peer(level, mask),
                )

            bulk.append(one) if later else one()
        sends.append((part[key], count - 1, *sems))

    def scatter_middle(key, later=False):
        level, _ = plan.scatters[key]
        index = scatter_keys.index(key)
        count = nx << level
        if plan.pre(key):
            wait_recv(first[key], count, scatter_send.at[index, 0], scatter_recv.at[index, 0])
            span = pl.ds(core * count, count)
            part[key][span] = part[key][span] + first[key][...]
            scatter_spread(key, count, later)

    def scatter_finish(key):
        level, _ = plan.scatters[key]
        index = scatter_keys.index(key)
        count = (nx << level) if plan.pre(key) else fronts << level
        wait_recv(landed[key], count - 1, scatter_send.at[index, 1], scatter_recv.at[index, 1])
        total = part[key][rank(level)]
        for place in range(count - 1):
            total = total + landed[key][place]
        return total

    def column_start(level):
        return fronts * pivots * ((1 << level) - 1)

    def update_start(level):
        return 2 * pivots * ((1 << level) - 1)

    loads = []
    for level in range(LEVELS):
        cols = pl.ds(column_start(level), (fronts * pivots) << level)
        loads.append(
            pltpu.make_async_copy(
                inverse_hbm.at[0, 0, :, cols], inverse_raw.at[:, cols], load_sem.at[level]
            )
        )
    loads.append(pltpu.make_async_copy(update_hbm.at[0, 0], update_raw, load_sem.at[LEVELS]))
    loads[0].start()
    loads[LEVELS].start()
    for level in range(1, LEVELS):
        loads[level].start()

    for level in range(LEVELS):
        gather_buffer["rhs", level][rhs_slot(level)] = rhs_ref[
            0, 0, :, level * pivots : (level + 1) * pivots
        ]

    @pl.when(column == 0)
    def _():
        for level in range(1, LEVELS):
            for slot in range(plan.size(level)):
                if rhs_block(level, slot) >> level >= 2:
                    gather_buffer["rhs", level][slot] = jnp.zeros((sides, pivots), F32)

    targets_ref[...] = jnp.zeros_like(targets_ref)
    targets_ref[:1, : lists_ref.shape[1]] = lists_ref[...]

    barrier = pltpu.get_barrier_semaphore()
    everyone = plan.size(LEVELS - 1)
    for mask in range(1, everyone):
        pl.semaphore_signal(
            barrier, inc=1, device_id=peer(LEVELS - 1, mask), device_id_type=MESH
        )
    pl.semaphore_wait(barrier, everyone - 1)

    for level in range(LEVELS - 1):
        send(
            targets_ref,
            targets_far.at[level],
            targets_send.at[level],
            targets_recv.at[level],
            (flip(leaf, 1 << level), front),
        )
    gather_start(("rhs", 0))
    for level in range(1, top):
        rhs_across(level)
    top_deep()

    def prepare(level):
        loads[level].wait()
        for block in range(column_start(level) // BLOCK, column_start(level + 1) // BLOCK):
            high, low = split(inverse_raw[:, block * BLOCK : (block + 1) * BLOCK])
            inverse_split[block, :pivots] = high
            inverse_split[block, pivots:] = low

    def inverse_columns(start, stop):
        blocks = range(start // BLOCK, stop // BLOCK)
        return jnp.concatenate([inverse_split[block] for block in blocks], 1)

    def prepare_update(level):
        cols = slice(update_start(level), update_start(level + 1))
        high, low = split(update_raw[:, cols])
        update_split[:pivots, cols] = high
        update_split[pivots:, cols] = low

    prepare(0)
    loads[LEVELS].wait()
    prepare_update(0)

    def swap(values):
        width = values.shape[1]
        even = lax.rem(lax.broadcasted_iota(jnp.int32, values.shape, 1), 2) == 0
        return jnp.where(
            even, pltpu.roll(values, width - 1, 1), pltpu.roll(values, 1, 1)
        )

    def pivot_coefficients():
        width = diagonal_ref.shape[2]
        from_pair = (
            lax.div(lax.broadcasted_iota(jnp.int32, (width // 2, width), 1), 2)
            == lax.broadcasted_iota(jnp.int32, (width // 2, width), 0)
        ).astype(F32)
        pair_rows = jnp.concatenate(
            [
                jnp.broadcast_to(coupling_ref[0], (8, width // 2)),
                jnp.broadcast_to(pairs_ref[0].astype(F32), (8, width // 2)),
            ],
            0,
        )
        repeated = jnp.dot(
            pair_rows, from_pair, precision=lax.Precision.HIGHEST, preferred_element_type=F32
        )
        couple, flags = repeated[:8], repeated[8:] > 0.5
        diagonal = jnp.broadcast_to(diagonal_ref[0], (8, width))

        other_diagonal = swap(diagonal)
        determinant = diagonal * other_diagonal - couple * couple
        straight = jnp.where(flags, other_diagonal / determinant, 1.0 / diagonal)[:1]
        crossed = jnp.where(flags, -couple / determinant, 0.0)[:1]
        return straight, crossed

    def pivot_solve(solved, level, straight, crossed):
        span = slice(level * pivots, (level + 1) * pivots)
        return solved * straight[:, span] + swap(solved) * crossed[:, span]

    def fetch_lists(levels, own):
        for level in levels:
            pltpu.make_async_remote_copy(
                targets_ref,
                targets_far.at[level],
                targets_send.at[level],
                targets_recv.at[level],
                device_id=(flip(leaf, 1 << level), front),
                device_id_type=MESH,
            ).wait()
        lists = [(targets_ref, 0)] if own else []
        lists += [(targets_far.at[level], level + 1) for level in levels]
        copies = [
            pltpu.make_async_copy(source, targets_smem.at[index], load_sem.at[LEVELS + 1 + index])
            for source, index in lists
        ]
        for copy in copies:
            copy.start()
        for copy in copies:
            copy.wait()

    def block_count(level):
        return 2 * pivots * (1 << level) // BLOCK

    def chosen_columns(level, child, index):
        place = update_start(level) // BLOCK + index
        upper = lax.rem(lax.div(leaf, 1 << level), 2)
        near, far = targets_smem[0, 0, place], targets_smem[level + 1, 0, place]
        block = near + (far - near) * (upper + child - 2 * upper * child)
        return inverse_split[column_start(level + 1) // BLOCK + block]

    def known_part(level):
        buffer = gather_buffer["rhs", level]
        product = None
        step = 2 if level else 1
        for slot in range(0, plan.size(level), step):
            values = jnp.concatenate([buffer[slot + i] for i in range(step)], 1)
            first_block = column_start(level) // BLOCK
            blocks = [first_block + rhs_block(level, slot + i) for i in range(step)]
            term = along_columns(
                rows_of(values),
                jnp.concatenate([inverse_split[block] for block in blocks], 1),
            )
            product = term if product is None else product + term
        return product

    def block_at(buffer, level, child, index, parent):
        halves = []
        for place in (2 * index, 2 * index + 1):
            slot = slot_of(level, place)
            if parent:
                rank_core, rest = divmod(slot, nx << level)
                rank_column, offset = divmod(rest, 1 << level)
                slot = (
                    rank_core * (nx << (level + 1))
                    + rank_column * (1 << (level + 1))
                    + (child << level)
                    + offset
                )
            halves.append(slot)
        return halves

    group, wide = nx << 1, nx
    corner = column * 2 + lax.rem(leaf, 2)
    pair_mask = group

    def side(index):
        return side_send.at[index], side_recv.at[index]

    def turned(level):
        cols = slice(update_start(level), update_start(level + 1))
        high, low = split(update_raw[:, cols].T)
        return jnp.concatenate(
            [jnp.concatenate([high, low], 1), jnp.concatenate([low, high], 1)], 0
        )

    def cross_start():
        left = turned(1)
        rows = left.shape[0] // 2
        for half_index in range(2):
            picks = []
            for i in range(wide):
                index, child = divmod(half_index * wide + i, 2)
                picks.append(chosen_columns(0, child, index))
            product = across(left, jnp.concatenate(picks, 1), rows)
            for block in range(group):
                for i in range(wide):
                    cross_part[half_index, block, i] = product[
                        block * pivots : (block + 1) * pivots, i * pivots : (i + 1) * pivots
                    ]
        send(cross_part.at[1 - core], cross_first, *side(0), peer(1, pair_mask))
        sends.append((cross_first, group, *side(0)))

    def cross_spread():
        wait_recv(cross_first, group, *side(0))
        for block in range(group):
            cross_part[core, block] = cross_part[core, block] + cross_first[block]
        for mask in far_first(group):
            send(
                cross_part.at[core, flip(corner, mask)],
                cross_landed.at[mask - 1],
                *side(1),
                peer(1, mask),
            )
        sends.append((cross_landed, group - 1, *side(1)))

    def cross_share():
        wait_recv(cross_landed, group - 1, *side(1))
        total = cross_part[core, corner]
        for place in range(group - 1):
            total = total + cross_landed[place]
        span = cross_row.at[pl.ds(core * wide, wide)]
        cross_row[pl.ds(core * wide, wide)] = total
        send(span, span, *side(2), peer(1, pair_mask))
        sends.append((cross_row, wide, *side(2)))

    def cross_rows():
        wait_recv(cross_row, wide, *side(2))
        for block in range(group):
            cols = slice(block * pivots, (block + 1) * pivots)
            high, low = split(cross_row[block])
            cross_row_split[:pivots, cols] = high
            cross_row_split[pivots:, cols] = low

    def cross_turn():
        for mask in far_first(group):
            send(
                cross_row.at[flip(corner, mask)], cross_col.at[corner], *side(3), peer(1, mask)
            )
        sends.append((cross_row, group - 1, *side(3)))
        cross_col[corner] = cross_row[corner]

    def cross_columns():
        wait_recv(cross_col, group - 1, *side(3))
        for block in range(group):
            high, low = split(cross_col[block])
            cross_col_split[block, :pivots] = high
            cross_col_split[block, pivots:] = low

    def low_start():
        left = turned(0)
        rows = left.shape[0] // 2
        for target in range(fronts):
            product = across(left, inverse_split[target], rows)
            for i in range(nx):
                low_part[target % 2, target // 2, i] = product[i * pivots : (i + 1) * pivots]
        send(low_part.at[1 - core], low_first, *side(4), peer(0, nx))
        sends.append((low_first, nx, *side(4)))

    def low_spread():
        wait_recv(low_first, nx, *side(4))
        for target in range(nx):
            low_part[core, target] = low_part[core, target] + low_first[target]
        for mask in range(1, nx):
            send(
                low_part.at[core, flip(column, mask)], low_landed.at[mask - 1], *side(5), peer(0, mask)
            )
        sends.append((low_landed, nx - 1, *side(5)))

    def low_finish():
        wait_recv(low_landed, nx - 1, *side(5))
        total = low_part[core, column]
        for place in range(nx - 1):
            total = total + low_landed[place]
        for i in range(nx):
            high, low = split(total[i])
            low_split[i, :pivots] = high
            low_split[i, pivots:] = low

    def sent_up(solved, level):
        key = ("up", level)
        start = update_start(level)
        blocks = block_count(level)
        partial = across(
            square_of(solved), update_split[:, start : start + blocks * BLOCK], sides
        )
        for index in range(blocks):
            for i, slot in enumerate(block_at(None, level, 0, index, False)):
                part[key][slot] = partial[
                    i * half : (i + 1) * half, index * BLOCK : (index + 1) * BLOCK
                ]
        scatter_start(key)

    def less_children(product, level):
        below = level - 1
        buffer = gather_buffer["up", below]
        for child in range(2):
            for index in range(0, block_count(below), 2):
                values, matrices = [], []
                for i in (index, index + 1):
                    low_slot, high_slot = block_at(buffer, below, child, i, True)
                    values.append(jnp.concatenate([buffer[low_slot], buffer[high_slot]], 0))
                    matrices.append(chosen_columns(below, child, i))
                product = product - along_columns(
                    rows_of(jnp.concatenate(values, 1)), jnp.concatenate(matrices, 1)
                )
        return product

    def sent_down(square, level):
        key = ("down", level - 1)
        for child in range(2):
            for index in range(0, block_count(level - 1), 2):
                matrix = jnp.concatenate(
                    [chosen_columns(level - 1, child, i) for i in (index, index + 1)], 1
                )
                partial = across(square, matrix, sides)
                for j in range(2):
                    places = block_at(None, level - 1, child, index + j, True)
                    for i, slot in enumerate(places):
                        part[key][slot] = partial[
                            i * half : (i + 1) * half, j * BLOCK : (j + 1) * BLOCK
                        ]
        scatter_start(key)

    def sent_out(square, level):
        out_key = ("out", level)
        step = 2 if level else 1
        for slot in range(0, plan.size(level), step):
            start = column_start(level) + slot_block(level, slot) * pivots
            partial = across(square, inverse_columns(start, start + step * pivots), sides)
            for i in range(step):
                part[out_key][slot + i] = partial[:, i * pivots : (i + 1) * pivots]
        scatter_start(out_key)

    def with_parent(level):
        buffer = gather_buffer["down", level]
        product = None
        for index in range(0, block_count(level), 2):
            values = []
            for i in (index, index + 1):
                low_slot, high_slot = block_at(buffer, level, 0, i, False)
                values.append(jnp.concatenate([buffer[low_slot], buffer[high_slot]], 0))
            start = update_start(level) + index * BLOCK
            term = along_columns(
                rows_of(jnp.concatenate(values, 1)),
                update_split[:, start : start + 2 * BLOCK],
            )
            product = term if product is None else product + term
        return weighted[level] - fold(product, sides, pivots)

    def own_core(key):
        return [gather_buffer[key][core * group + block] for block in range(group)]

    weighted = []
    prepare(1)
    prepare_update(1)
    fetch_lists([0], True)
    cross_start()
    gather_finish(("rhs", 0))
    solved = fold(known_part(0), sides, pivots)
    sent_up(solved, 0)
    rhs_beside(1)
    rhs_beside(2)
    cross_spread()
    fetch_lists(list(range(1, LEVELS - 1)), False)
    coefficients = pivot_coefficients()
    weighted.append(pivot_solve(solved, 0, *coefficients))
    total = scatter_finish(("up", 0))
    gather_buffer["up", 0][rank(1)] = total
    gather_start(("up", 0))
    rhs_deep(2)
    rhs_relay(1)
    prepare(2)
    prepare_update(2)
    rhs_finish(1)
    known = known_part(1)
    sent_up(fold(known, sides, pivots), 1)
    low_start()
    scatter_middle(("up", 1))
    top_first()
    gather_forward(("up", 0))
    cross_share()
    total = scatter_finish(("up", 1))
    cross_rows()
    total = total - fold(
        along_columns(
            rows_of(jnp.concatenate(own_core(("up", 0)), 1)), cross_row_split[...]
        ),
        half,
        pivots,
    )
    gather_buffer["up", 1][rank(2)] = total
    gather_start(("up", 1))
    top_second()
    gather_finish(("up", 0))
    solved = fold(less_children(known, 1), sides, pivots)
    weighted.append(pivot_solve(solved, 1, *coefficients))
    rhs_relay(2)
    rhs_finish(2)
    product = known_part(2)
    gather_forward(("up", 1))
    prepare(3)

    for level in range(2, LEVELS):
        below = level - 1
        gather_finish(("up", below))
        solved = fold(less_children(product, level), sides, pivots)
        if level + 1 < LEVELS:
            key = ("up", level)
            sent_up(solved, level)
            weighted.append(pivot_solve(solved, level, *coefficients))
            scatter_middle(key)
            cross_turn()
            top_relay()
            total = scatter_finish(key)
            gather_buffer[key][rank(level + 1)] = total
            gather_start(key)
            rhs_finish(level + 1)
            low_spread()
            sent_down(square_of(weighted[1]), 1)
            product = known_part(level + 1)
            scatter_middle(("down", 0))
            gather_forward(key)
        else:
            weighted.append(pivot_solve(solved, level, *coefficients))

    for level in range(LEVELS - 1, 1, -1):
        target = weighted[level]
        if level + 1 < LEVELS:
            gather_finish(("down", level))
            target = with_parent(level)
        square = square_of(target)
        key = ("down", level - 1)
        out_key = ("out", level)
        sent_down(square, level)
        scatter_middle(key)
        issue(SHARE)
        if level == LEVELS - 1:
            sent_out(square_of(weighted[0]), 0)
        sent_out(square, level)
        if level == 2:
            cross_columns()
            low_finish()
            out_ref[0, 0, :, :pivots] = scatter_finish(("out", 0))
            gather_buffer["down", 0][rank(0)] = scatter_finish(("down", 0))
        total = scatter_finish(key)
        gather_buffer[key][rank(level - 1)] = total
        gather_start(key)
        scatter_middle(out_key, later=True)
        issue(SHARE if level > 2 else len(bulk))
        gather_forward(key)
        if level > 2:
            issue(SHARE)

    total = gather_buffer["down", 0][rank(0)]
    for block, values in enumerate(own_core(("down", 1))):
        total = total - across(square_of(values), cross_col_split[block], half)
    gather_buffer["down", 0][rank(0)] = total
    gather_start(("down", 0))
    gather_finish(("down", 1))
    sent_out(square_of(with_parent(1)), 1)
    scatter_middle(("out", 1))
    gather_finish(("down", 0))
    buffer = gather_buffer["down", 0]
    total = out_ref[0, 0, :, :pivots]
    for index in range(block_count(0)):
        low_slot, high_slot = block_at(buffer, 0, 0, index, False)
        values = jnp.concatenate([buffer[low_slot], buffer[high_slot]], 0)
        total = total - across(square_of(values), low_split[index], sides)
    out_ref[0, 0, :, :pivots] = total
    for level in range(LEVELS - 1, 0, -1):
        out_ref[0, 0, :, level * pivots : (level + 1) * pivots] = scatter_finish(("out", level))
    for item in sends:
        wait_send(*item)
    for level in range(1, top):
        rhs_drain(level)
    top_drain()


def per_device(*arguments):
    (
        right_side,
        factor_inverse,
        update_panel,
        update_targets,
        pivot_pairs,
        pivot_diagonal,
        pivot_coupling,
    ) = arguments
    pivots = factor_inverse.shape[2]
    sides = right_side.shape[2]
    fronts = lax.axis_size("front")
    plan = Plan(fronts, sides)
    nx = fronts // 2
    group, wide = nx << 1, nx
    targets = jax.ShapeDtypeStruct((8, BLOCK), jnp.int32)
    buffers = []
    for level, rows in plan.gathers.values():
        buffers.append(pltpu.VMEM((plan.size(level), rows, pivots), F32))
    for key, (level, rows) in plan.scatters.items():
        buffers.append(pltpu.VMEM((plan.size(level), rows, pivots), F32))
        buffers.append(pltpu.VMEM((plan.size(level), rows, pivots), F32))
        if plan.pre(key):
            buffers.append(pltpu.VMEM((nx << level, rows, pivots), F32))
    vmem = pl.BlockSpec(memory_space=pltpu.VMEM)
    hbm = pl.BlockSpec(memory_space=pl.ANY)
    dma = pltpu.SemaphoreType.DMA
    return pl.pallas_call(
        functools.partial(kernel, plan, pivots),
        out_shape=pltpu.VMEM(right_side.shape, F32),
        in_specs=[vmem, hbm, hbm, vmem, vmem, vmem, vmem],
        out_specs=vmem,
        scratch_shapes=[
            pltpu.VMEM(factor_inverse.shape[2:], F32),
            pltpu.VMEM(update_panel.shape[2:], F32),
            pltpu.VMEM((factor_inverse.shape[3] // BLOCK, 2 * pivots, BLOCK), BF16),
            pltpu.VMEM((2 * pivots, update_panel.shape[3]), BF16),
            pltpu.VMEM(targets.shape, jnp.int32),
            pltpu.VMEM((LEVELS - 1,) + targets.shape, jnp.int32),
            pltpu.SMEM((LEVELS,) + targets.shape, jnp.int32),
            dma((2 * LEVELS + 1,)),
            dma((LEVELS - 1,)),
            dma((LEVELS - 1,)),
            dma((len(plan.gathers), 2)),
            dma((len(plan.gathers), 2)),
            dma((len(plan.scatters), 2)),
            dma((len(plan.scatters), 2)),
            dma((LEVELS, 4)),
            dma((LEVELS, 4)),
            dma((6,)),
            dma((6,)),
            pltpu.VMEM((2, group, wide, pivots, pivots), F32),
            pltpu.VMEM((group, wide, pivots, pivots), F32),
            pltpu.VMEM((group - 1, wide, pivots, pivots), F32),
            pltpu.VMEM((group, pivots, pivots), F32),
            pltpu.VMEM((group, pivots, pivots), F32),
            pltpu.VMEM((2 * pivots, group * pivots), BF16),
            pltpu.VMEM((group, 2 * pivots, pivots), BF16),
            pltpu.VMEM((2, nx, nx, pivots, pivots), F32),
            pltpu.VMEM((nx, nx, pivots, pivots), F32),
            pltpu.VMEM((nx - 1, nx, pivots, pivots), F32),
            pltpu.VMEM((nx, 2 * pivots, pivots), BF16),
            *buffers,
        ],
        compiler_params=pltpu.CompilerParams(collective_id=0, has_side_effects=True),
    )(
        right_side,
        factor_inverse,
        update_panel,
        update_targets,
        pivot_pairs,
        pivot_diagonal,
        pivot_coupling,
    )


def solution(mesh):
    in_specs = (
        P("leaf", "front", None, None),
        P("leaf", "front", None, None),
        P("leaf", "front", None, None),
        P("leaf", None),
        P("leaf", "front", None),
        P("leaf", "front", None),
        P("leaf", "front", None),
    )
    out_specs = P("leaf", "front", None, None)
    return jax.shard_map(
        per_device, mesh=mesh, in_specs=in_specs, out_specs=out_specs, check_vma=False
    )
```

```python
import functools

import jax
import jax.numpy as jnp
from jax import lax
from jax.experimental import pallas as pl
from jax.experimental.pallas import tpu as pltpu
from jax.sharding import PartitionSpec as P

LEVELS = 4
BLOCK = 128
TOP = LEVELS - 1
DEPTH = 1 << TOP - 1
MESH = pl.DeviceIdType.MESH
F32 = jnp.float32
BF16 = jnp.bfloat16


def flip(value, mask):
    result = value
    bit = 0
    while mask >> bit:
        if mask >> bit & 1:
            unit = 1 << bit
            result = result + (1 - 2 * lax.rem(lax.div(value, unit), 2)) * unit
        bit += 1
    return result


def split(values):
    high = values.astype(BF16)
    return high, (values - high.astype(F32)).astype(BF16)


def rows_of(values):
    high, low = split(values)
    return jnp.concatenate([high, low], 0)


def square_of(values):
    rows = rows_of(values)
    pieces = []
    for start in range(0, rows.shape[1], BLOCK):
        pieces += [rows[:, start : start + BLOCK]] * 2
    return jnp.concatenate(pieces, 1)


def along_columns(stacked, matrix):
    return lax.dot_general(
        stacked, matrix, (((1,), (1,)), ((), ())), preferred_element_type=F32
    )


def fold(product):
    sides = product.shape[0] // 2
    both = product[:sides] + product[sides:]
    pieces = []
    for start in range(0, both.shape[1], 2 * BLOCK):
        pieces.append(
            both[:, start : start + BLOCK] + both[:, start + BLOCK : start + 2 * BLOCK]
        )
    return jnp.concatenate(pieces, 1)


def across(square, matrix):
    product = jnp.dot(square, matrix, preferred_element_type=F32)
    half = product.shape[0] // 2
    return product[:half] + product[half:]


def far_first(count):
    return sorted(range(1, count), key=lambda mask: -bin(mask).count("1"))


def kernel(nx, pivots, keys, *refs):
    (
        rhs_ref,
        inverse_hbm,
        update_hbm,
        lists_ref,
        pairs_ref,
        diagonal_ref,
        coupling_ref,
        out_ref,
        inverse_raw,
        update_raw,
        inverse_split,
        update_split,
        coefficients,
        targets_ref,
        targets_far,
        targets_smem,
        result_near,
        result_far,
        cross_part,
        cross_landed,
        cross_row,
        cross_col,
        cross_row_split,
        cross_col_split,
        low_part,
        low_landed,
        low_sum,
        low_split,
        load_sem,
        targets_send,
        targets_recv,
        weight_send,
        weight_recv,
        side_send,
        side_recv,
        rhs_send,
        rhs_recv,
        out_send,
        out_recv,
        swap_send,
        swap_recv,
        gather_send,
        gather_recv,
        scatter_send,
        scatter_recv,
        *buffers,
    ) = refs
    half = rhs_ref.shape[2] // 2
    leaf = lax.axis_index("leaf")
    front = lax.axis_index("front")
    core, column = lax.rem(front, 2), lax.div(front, 2)
    row = lax.rem(leaf, 2)
    buffers = list(buffers)
    rhs = [buffers.pop(0) for _ in range(LEVELS)]
    out_part = [buffers.pop(0) for _ in range(LEVELS)]
    out_landed = [buffers.pop(0) for _ in range(LEVELS)]
    gathered, part, landed = {}, {}, {}
    for key in keys:
        gathered[key] = buffers.pop(0)
        part[key] = buffers.pop(0)
        landed[key] = buffers.pop(0)

    def chips(level):
        return nx << level

    def rank(level):
        return column * (1 << level) + lax.rem(leaf, 1 << level)

    def peer(level, mask, other_core=False):
        near = 1 - core if other_core else core
        return flip(leaf, mask % (1 << level)), flip(column, (mask >> level) % nx) * 2 + near

    partner = (leaf, column * 2 + 1 - core)

    def slot_at(level, child, block):
        slot_column, offset = divmod(block, 1 << level)
        return (slot_column << level + 1) + (child << level) + offset

    def slot(level):
        inside = lax.rem(leaf, 1 << level)
        if level == TOP:
            return (row * nx + column) * DEPTH + lax.div(inside, 2)
        if level < 2:
            return rank(level)
        return lax.div(inside, 2) * (2 * nx) + column * 2 + row

    def slot_place(level, index):
        if level == TOP:
            rest, deep = divmod(index, DEPTH)
            slot_row, slot_column = divmod(rest, nx)
        elif level < 2:
            slot_column, offset = divmod(index, 1 << level)
            deep, slot_row = divmod(offset, 2)
        else:
            deep, rest = divmod(index, 2 * nx)
            slot_column, slot_row = divmod(rest, 2)
        return slot_column, deep * 2 + slot_row

    def slot_blocks(level, index):
        slot_column, offset = slot_place(level, index)
        first = column_start(level) // BLOCK
        return [first + ((slot_column * 2 + parity) << level) + offset for parity in range(2)]

    def column_start(level):
        return 2 * nx * pivots * ((1 << level) - 1)

    def update_start(level):
        return 2 * pivots * ((1 << level) - 1)

    def block_count(level):
        return 2 * pivots * (1 << level) // BLOCK

    sends = []

    def send(source, target, sems, device):
        pltpu.make_async_remote_copy(
            source, target, *sems, device_id=device, device_id_type=MESH
        ).start()

    def span_copy(buffer, count, sems):
        span = buffer.at[pl.ds(0, count)]
        return pltpu.make_async_remote_copy(
            span, span, *sems, device_id=partner, device_id_type=MESH
        )

    def wait_recv(buffer, count, sems):
        span_copy(buffer, count, sems).wait_recv()

    def wait_send(buffer, count, sems):
        span_copy(buffer, count, sems).wait_send()

    def on(slot_column, slot_core=None):
        if slot_core is None:
            return pl.when(column == slot_column)
        return pl.when((column == slot_column) & (core == slot_core))

    def for_column(body):
        for index in range(nx):

            @on(index)
            def _():
                body(index)

    loads = []
    for level in range(LEVELS):
        cols = pl.ds(column_start(level), column_start(level + 1) - column_start(level))
        loads.append(
            pltpu.make_async_copy(
                inverse_hbm.at[0, 0, :, cols], inverse_raw.at[core, :, cols], load_sem.at[level]
            )
        )
    loads.append(
        pltpu.make_async_copy(update_hbm.at[0, 0], update_raw.at[core], load_sem.at[LEVELS])
    )
    for index in (0, LEVELS, *range(1, LEVELS)):
        loads[index].start()

    mine = pl.ds(core * half, half)
    theirs = pl.ds((1 - core) * half, half)

    def level_cols(level):
        return slice(level * pivots, (level + 1) * pivots)

    for level in range(LEVELS):
        rhs[level][slot(level), core] = rhs_ref[0, 0, mine, level_cols(level)]

    @on(0)
    def _():
        zeros = jnp.zeros((2, half, pivots), F32)
        for level in range(1, LEVELS):
            for index in range(chips(level)):
                if slot_place(level, index)[0]:
                    rhs[level][index] = zeros

    @on(1)
    def _():
        zeros = jnp.zeros((2, half, pivots), F32)
        for level in range(2):
            for place in range((1 << level) - 1, chips(level) - 1):
                out_landed[level][place] = zeros

    targets_ref[...] = jnp.zeros_like(targets_ref)
    targets_ref[:1, : lists_ref.shape[1]] = lists_ref[...]

    def swap(values):
        width = values.shape[1]
        even = lax.rem(lax.broadcasted_iota(jnp.int32, values.shape, 1), 2) == 0
        return jnp.where(
            even, pltpu.roll(values, width - 1, 1), pltpu.roll(values, 1, 1)
        )

    def pivot_coefficients():
        width = diagonal_ref.shape[2]
        from_pair = (
            lax.div(lax.broadcasted_iota(jnp.int32, (width // 2, width), 1), 2)
            == lax.broadcasted_iota(jnp.int32, (width // 2, width), 0)
        ).astype(F32)
        pair_rows = jnp.concatenate(
            [
                jnp.broadcast_to(coupling_ref[0], (8, width // 2)),
                jnp.broadcast_to(pairs_ref[0].astype(F32), (8, width // 2)),
            ],
            0,
        )
        repeated = jnp.dot(
            pair_rows, from_pair, precision=lax.Precision.HIGHEST, preferred_element_type=F32
        )
        couple, flags = repeated[:8], repeated[8:] > 0.5
        diagonal = jnp.broadcast_to(diagonal_ref[0], (8, width))

        other_diagonal = swap(diagonal)
        determinant = diagonal * other_diagonal - couple * couple
        straight = jnp.where(flags, other_diagonal / determinant, 1.0 / diagonal)
        crossed = jnp.where(flags, -couple / determinant, 0.0)
        coefficients[core, 0] = straight
        coefficients[core, 1] = crossed

    def pivot_solve(solved, level):
        straight, crossed = [
            jnp.concatenate(
                [coefficients[parity, kind, :1, level_cols(level)] for parity in range(2)], 1
            )
            for kind in range(2)
        ]
        return solved * straight + swap(solved) * crossed

    barrier = pltpu.get_barrier_semaphore()
    everyone = [
        (flip(leaf, mask % (2 * DEPTH)), flip(front, mask // (2 * DEPTH)))
        for mask in range(1, 4 * nx * DEPTH)
    ]
    for device in everyone:
        pl.semaphore_signal(barrier, inc=1, device_id=device, device_id_type=MESH)
    pivot_coefficients()
    pl.semaphore_wait(barrier, len(everyone))

    def list_sems(level):
        return targets_send.at[level], targets_recv.at[level]

    def list_copy(level):
        return pltpu.make_async_remote_copy(
            targets_ref,
            targets_far.at[level],
            *list_sems(level),
            device_id=(flip(leaf, 1 << level), front),
            device_id_type=MESH,
        )

    def rhs_sems(level, phase):
        return rhs_send.at[level, phase], rhs_recv.at[level, phase]

    def weight_sems(index):
        return weight_send.at[index], weight_recv.at[index]

    def rhs_base():
        sems = rhs_sems(0, 0)
        target = rhs[0].at[column, core]
        source = rhs_ref.at[0, 0]
        for mask in range(1, nx):
            for each, there in ((mine, core), (theirs, 1 - core)):
                send(
                    source.at[each, pl.ds(0, pivots)],
                    target,
                    sems,
                    (leaf, flip(column, mask) * 2 + there),
                )
        send(source.at[theirs, pl.ds(0, pivots)], target, sems, partner)
        sends.append((rhs[0].at[0], 1, sems))
        sends.append((rhs[0], nx - 1, sems))

    def rhs_halves():
        for level in range(1, LEVELS):
            send(
                rhs_ref.at[0, 0, theirs, pl.ds(level * pivots, pivots)],
                rhs[level].at[slot(level), core],
                rhs_sems(level, 3),
                partner,
            )
            sends.append((rhs[level].at[0], 1, rhs_sems(level, 3)))

    def give_inverse(level):
        loads[level].wait()
        cols = pl.ds(column_start(level), column_start(level + 1) - column_start(level))
        span = inverse_raw.at[core, :, cols]
        copy = pltpu.make_async_remote_copy(
            span, span, *weight_sems(level), device_id=partner, device_id_type=MESH
        )
        copy.start()
        return copy

    def give_update(level):
        if not level:
            loads[LEVELS].wait()
        cols = pl.ds(update_start(level), update_start(level + 1) - update_start(level))
        span = update_raw.at[core, :, cols]
        copy = pltpu.make_async_remote_copy(
            span, span, *weight_sems(LEVELS + level), device_id=partner, device_id_type=MESH
        )
        copy.start()
        return copy

    list_copies = [list_copy(level) for level in range(LEVELS - 1)]
    rhs_base()
    for copy in list_copies:
        copy.start()
    rhs_halves()
    given, given_update = {}, {}
    given[0] = give_inverse(0)
    given_update[0] = give_update(0)
    given[1] = give_inverse(1)
    given_update[1] = give_update(1)
    coefficient_copy = pltpu.make_async_remote_copy(
        coefficients.at[core],
        coefficients.at[core],
        *weight_sems(2 * LEVELS),
        device_id=partner,
        device_id_type=MESH,
    )
    coefficient_copy.start()
    given[2] = give_inverse(2)
    given_update[2] = give_update(2)
    given[3] = give_inverse(3)

    def prepare(level):
        given[level].wait_recv()
        for block in range(column_start(level) // BLOCK, column_start(level + 1) // BLOCK):
            for parity in range(2):
                high, low = split(inverse_raw[parity, :, block * BLOCK : (block + 1) * BLOCK])
                start = parity * 2 * pivots
                inverse_split[block, start : start + pivots] = high
                inverse_split[block, start + pivots : start + 2 * pivots] = low

    def prepare_update(level):
        given_update[level].wait_recv()
        cols = slice(update_start(level), update_start(level + 1))
        for parity in range(2):
            high, low = split(update_raw[parity, :, cols])
            start = parity * 2 * pivots
            update_split[start : start + pivots, cols] = high
            update_split[start + pivots : start + 2 * pivots, cols] = low

    def fetch_lists(levels, own):
        for level in levels:
            list_copies[level].wait()
        lists = [(targets_ref, 0)] if own else []
        lists += [(targets_far.at[level], level + 1) for level in levels]
        copies = [
            pltpu.make_async_copy(source, targets_smem.at[index], load_sem.at[LEVELS + 1 + index])
            for source, index in lists
        ]
        for copy in copies:
            copy.start()
        for copy in copies:
            copy.wait()

    def half_ready(level):
        wait_recv(rhs[level].at[0], 1, rhs_sems(level, 3))

    def base_ready():
        wait_recv(rhs[0].reshape(nx * 2, half, pivots), 2 * nx - 1, rhs_sems(0, 0))

    def one_across():
        half_ready(1)

        @on(0)
        def _():
            each = rhs[1].at[rank(1)]
            send(each, each, rhs_sems(1, 0), peer(1, 2))

    def one_beside():
        def body(index):
            if index:
                wait_recv(rhs[1], index, rhs_sems(1, 0))
            for back in range(index + 1):
                each = rhs[1].at[rank(1) - 2 * back]
                send(each, each, rhs_sems(1, 1), peer(1, 1))

        for_column(body)

    def one_ready():
        for_column(lambda index: wait_recv(rhs[1], index + 1, rhs_sems(1, 1)))

    def pair_start():
        return lax.rem(lax.div(leaf, 2), 2) * (2 * nx)

    def two_beside():
        half_ready(2)
        each = rhs[2].at[slot(2)]
        send(each, each, rhs_sems(2, 1), peer(2, 1))
        sends.append((rhs[2], 1, rhs_sems(2, 1)))

    def two_across():
        wait_recv(rhs[2], 1, rhs_sems(2, 1))

        @on(0)
        def _():
            span = rhs[2].at[pl.ds(pair_start(), 2)]
            send(span, span, rhs_sems(2, 0), peer(2, 4))

    def two_deep():
        def body(index):
            if index:
                wait_recv(rhs[2], 2 * index, rhs_sems(2, 0))
            span = rhs[2].at[pl.ds(pair_start(), 2 * (index + 1))]
            send(span, span, rhs_sems(2, 2), peer(2, 2))

        for_column(body)

    def two_ready():
        for_column(lambda index: wait_recv(rhs[2], 2 * (index + 1), rhs_sems(2, 2)))

    def top_run(slot_row, slot_column):
        return rhs[TOP].at[pl.ds((slot_row * nx + slot_column) * DEPTH, DEPTH)]

    def top_deep():
        half_ready(TOP)
        each = rhs[TOP].at[slot(TOP)]
        for deep in range(DEPTH - 1, 0, -1):
            send(each, each, rhs_sems(TOP, 0), peer(TOP, 2 * deep))
        sends.append((rhs[TOP], DEPTH - 1, rhs_sems(TOP, 0)))

    def top_beside():
        run = top_run(row, column)
        send(run, run, rhs_sems(TOP, 2), peer(TOP, 1))

    def top_first():
        wait_recv(rhs[TOP], DEPTH - 1, rhs_sems(TOP, 0))

        @pl.when(core == 1)
        def _():
            top_beside()

        @on(0, 0)
        def _():
            run = top_run(row, 0)
            send(run, run, rhs_sems(TOP, 1), peer(TOP, 1 << TOP))

        sends.append((rhs[TOP], DEPTH, rhs_sems(TOP, 2)))

    def top_second():
        @pl.when(core == 0)
        def _():
            top_beside()

        @on(0, 1)
        def _():
            wait_recv(rhs[TOP], DEPTH, rhs_sems(TOP, 2))
            for each in range(2):
                run = top_run(each, 0)
                send(run, run, rhs_sems(TOP, 1), peer(TOP, 1 << TOP))

        @on(1, 0)
        def _():
            wait_recv(rhs[TOP], DEPTH, rhs_sems(TOP, 1))
            run = top_run(row, 0)
            send(run, run, rhs_sems(TOP, 2), peer(TOP, 1))

    def top_ready():
        @on(0, 0)
        def _():
            wait_recv(rhs[TOP], DEPTH, rhs_sems(TOP, 2))

        @on(1, 0)
        def _():
            wait_recv(rhs[TOP], 2 * DEPTH, rhs_sems(TOP, 2))

        @on(1, 1)
        def _():
            wait_recv(rhs[TOP], DEPTH, rhs_sems(TOP, 2))
            wait_recv(rhs[TOP], 2 * DEPTH, rhs_sems(TOP, 1))

    def rhs_drain():
        def body(index):
            if not index:
                wait_send(rhs[1], 1, rhs_sems(1, 0))
                wait_send(rhs[2], 2, rhs_sems(2, 0))
            wait_send(rhs[1], index + 1, rhs_sems(1, 1))
            wait_send(rhs[2], 2 * (index + 1), rhs_sems(2, 2))

        for_column(body)

        @on(0, 0)
        def _():
            wait_send(rhs[TOP], DEPTH, rhs_sems(TOP, 1))

        @on(0, 1)
        def _():
            wait_send(rhs[TOP], 2 * DEPTH, rhs_sems(TOP, 1))

        @on(1, 0)
        def _():
            wait_send(rhs[TOP], DEPTH, rhs_sems(TOP, 2))

    def group_of(key):
        return key[1] + (1 if key[0] == "up" else 0), key[1] + (0 if key[0] == "up" else 1)

    def key_sems(kind, key):
        index = keys.index(key)
        if kind == "gather":
            return gather_send.at[index], gather_recv.at[index]
        return scatter_send.at[index], scatter_recv.at[index]

    def gather_start(key, total):
        level, _ = group_of(key)
        buffer, sems = gathered[key], key_sems("gather", key)
        buffer[rank(level)] = total
        for mask in far_first(chips(level)):
            each = buffer.at[rank(level)]
            send(each, each, sems, peer(level, mask))
        sends.append((buffer, chips(level) - 1, sems))

    def gather_finish(key):
        level, _ = group_of(key)
        wait_recv(gathered[key], chips(level) - 1, key_sems("gather", key))

    def scatter_start(key):
        _, level = group_of(key)
        sems = key_sems("scatter", key)
        for mask in far_first(chips(level)):
            send(
                part[key].at[flip(rank(level), mask)],
                landed[key].at[mask - 1],
                sems,
                peer(level, mask),
            )
        sends.append((part[key], chips(level) - 1, sems))

    def scatter_finish(key):
        _, level = group_of(key)
        wait_recv(landed[key], chips(level) - 1, key_sems("scatter", key))
        total = part[key][rank(level)]
        for place in range(chips(level) - 1):
            total = total + landed[key][place]
        return total

    def chosen_columns(level, child, index):
        place = update_start(level) // BLOCK + index
        upper = lax.rem(lax.div(leaf, 1 << level), 2)
        near, far = targets_smem[0, 0, place], targets_smem[level + 1, 0, place]
        block = near + (far - near) * (upper + child - 2 * upper * child)
        return inverse_split[column_start(level + 1) // BLOCK + block]

    def known_part(level):
        product = None
        for index in range(chips(level)):
            values = jnp.concatenate([rhs[level][index, parity] for parity in range(2)], 1)
            matrix = jnp.concatenate(
                [inverse_split[block] for block in slot_blocks(level, index)], 1
            )
            term = along_columns(rows_of(values), matrix)
            product = term if product is None else product + term
        return product

    def sent_up(solved, level):
        start, blocks = update_start(level), block_count(level)
        partial = across(square_of(solved), update_split[:, start : start + blocks * BLOCK])
        for block in range(blocks):
            part["up", level][block] = partial[:, block * BLOCK : (block + 1) * BLOCK]
        scatter_start(("up", level))

    def less_children(product, level):
        below = level - 1
        buffer = gathered["up", below]
        for child in range(2):
            for index in range(0, block_count(below), 2):
                pair = (index, index + 1)
                values = [buffer[slot_at(below, child, i)] for i in pair]
                matrices = [chosen_columns(below, child, i) for i in pair]
                product = product - along_columns(
                    rows_of(jnp.concatenate(values, 1)), jnp.concatenate(matrices, 1)
                )
        return product

    def sent_down(square, level):
        key = ("down", level - 1)
        for child in range(2):
            for index in range(0, block_count(level - 1), 2):
                pair = (index, index + 1)
                matrix = jnp.concatenate(
                    [chosen_columns(level - 1, child, i) for i in pair], 1
                )
                partial = across(square, matrix)
                for j, i in enumerate(pair):
                    part[key][slot_at(level - 1, child, i)] = partial[
                        :, j * BLOCK : (j + 1) * BLOCK
                    ]
        scatter_start(key)

    def with_parent(level):
        buffer = gathered["down", level]
        product = None
        for index in range(0, block_count(level), 2):
            values = jnp.concatenate([buffer[index], buffer[index + 1]], 1)
            start = update_start(level) + index * BLOCK
            term = along_columns(rows_of(values), update_split[:, start : start + 2 * BLOCK])
            product = term if product is None else product + term
        return weighted[level] - fold(product)

    def out_sems(level, phase):
        return out_send.at[level, phase], out_recv.at[level, phase]

    def made_out(square, level):
        for index in range(chips(level)):
            matrix = jnp.concatenate(
                [inverse_split[block] for block in slot_blocks(level, index)], 1
            )
            partial = across(square, matrix)
            for parity in range(2):
                out_part[level][index, parity] = partial[
                    :, parity * pivots : (parity + 1) * pivots
                ]

    def plain_out_start(level):
        sems = out_sems(level, 0)

        def one(mask):
            send(
                out_part[level].at[flip(rank(level), mask)],
                out_landed[level].at[mask - 1],
                sems,
                peer(level, mask),
            )

        @on(1)
        def _():
            for mask in far_first(chips(level)):
                if mask >> level:
                    one(mask)

        for mask in far_first(1 << level):
            one(mask)

    def plain_out_finish(level):
        def body(index):
            fewer = chips(level) if index == 0 else 1 << level
            if fewer > 1:
                wait_recv(out_landed[level], fewer - 1, out_sems(level, 0))

        for_column(body)
        total = out_part[level][rank(level)]
        for place in range(chips(level) - 1):
            total = total + out_landed[level][place]
        return total

    def plain_out_drain(level):
        def body(index):
            fewer = chips(level) if index else 1 << level
            if fewer > 1:
                wait_send(out_landed[level], fewer - 1, out_sems(level, 0))

        for_column(body)

    def out_add(level, start, place, count):
        span = pl.ds(start, count)
        out_part[level][span] = out_part[level][span] + out_landed[level][place : place + count]

    def middle_first():
        other = (1 - lax.rem(lax.div(leaf, 2), 2)) * (2 * nx)

        def body(index):
            each = 2 * (index + 1)
            send(
                out_part[2].at[pl.ds(other, each)],
                out_landed[2].at[pl.ds(0, each)],
                out_sems(2, 0),
                peer(2, 2),
            )

        for_column(body)

    def middle_second():
        def body(index):
            each = 2 * (index + 1)
            wait_recv(out_landed[2], each, out_sems(2, 0))
            out_add(2, pair_start(), 0, each)
            if index:
                send(
                    out_part[2].at[pl.ds(pair_start(), 2)],
                    out_landed[2].at[pl.ds(2 * nx, 2)],
                    out_sems(2, 1),
                    peer(2, 4),
                )

        for_column(body)

    def middle_third():
        @on(0)
        def _():
            wait_recv(out_landed[2], 2, out_sems(2, 1))
            out_add(2, pair_start(), 2 * nx, 2)

        send(
            out_part[2].at[pair_start() + column * 2 + (1 - row)],
            out_landed[2].at[2 * nx + 2],
            out_sems(2, 2),
            peer(2, 1),
        )
        sends.append((out_landed[2], 1, out_sems(2, 2)))

    def middle_finish():
        wait_recv(out_landed[2], 1, out_sems(2, 2))
        return out_part[2][slot(2)] + out_landed[2][2 * nx + 2]

    def middle_drain():
        def body(index):
            wait_send(out_landed[2], 2 * (index + 1), out_sems(2, 0))
            if index:
                wait_send(out_landed[2], 2, out_sems(2, 1))

        for_column(body)

    def final_index(slot_row, slot_column):
        return (slot_row * nx + slot_column) * DEPTH

    def final_run(slot_row, slot_column, count=1):
        return out_part[TOP].at[pl.ds(final_index(slot_row, slot_column), count * DEPTH)]

    def final_first():
        for index in range(nx):

            @on(index, 0)
            def _():
                send(
                    final_run(1 - row, 0, index + 1),
                    out_landed[TOP].at[pl.ds(0, (index + 1) * DEPTH)],
                    out_sems(TOP, 0),
                    peer(TOP, 1),
                )

        @on(1, 1)
        def _():
            for each in range(2):
                send(
                    final_run(each, 0),
                    out_landed[TOP].at[pl.ds(each * DEPTH, DEPTH)],
                    out_sems(TOP, 0),
                    peer(TOP, 1 << TOP),
                )

    def final_second():
        there = out_landed[TOP].at[pl.ds(2 * DEPTH, DEPTH)]
        for index in range(nx):

            @on(index, 0)
            def _():
                wait_recv(out_landed[TOP], (index + 1) * DEPTH, out_sems(TOP, 0))
                out_add(TOP, final_index(row, 0), 0, (index + 1) * DEPTH)

        @on(1, 0)
        def _():
            send(final_run(row, 0), there, out_sems(TOP, 1), peer(TOP, 1 << TOP))

        @on(0, 1)
        def _():
            wait_recv(out_landed[TOP], 2 * DEPTH, out_sems(TOP, 0))
            for each in range(2):
                out_add(TOP, final_index(each, 0), each * DEPTH, DEPTH)

        @pl.when(core == 1)
        def _():
            send(final_run(1 - row, column), there, out_sems(TOP, 1), peer(TOP, 1))

    def final_third():
        @pl.when((core == 1) | (column == 0))
        def _():
            wait_recv(out_landed[TOP], DEPTH, out_sems(TOP, 1))
            out_add(TOP, final_index(row, column), 2 * DEPTH, DEPTH)

        deep = lax.rem(lax.div(leaf, 2), DEPTH)
        for mask in range(DEPTH - 1, 0, -1):
            send(
                out_part[TOP].at[final_index(row, column) + flip(deep, mask)],
                out_landed[TOP].at[3 * DEPTH + mask - 1],
                out_sems(TOP, 2),
                peer(TOP, 2 * mask),
            )
        sends.append((out_landed[TOP], DEPTH - 1, out_sems(TOP, 2)))

    def final_finish():
        wait_recv(out_landed[TOP], DEPTH - 1, out_sems(TOP, 2))
        total = out_part[TOP][slot(TOP)]
        for place in range(DEPTH - 1):
            total = total + out_landed[TOP][3 * DEPTH + place]
        return total

    def final_drain():
        for index in range(nx):

            @on(index, 0)
            def _():
                wait_send(out_landed[TOP], (index + 1) * DEPTH, out_sems(TOP, 0))

        @on(1, 1)
        def _():
            wait_send(out_landed[TOP], 2 * DEPTH, out_sems(TOP, 0))

        @pl.when((core == 1) | (column == 1))
        def _():
            wait_send(out_landed[TOP], DEPTH, out_sems(TOP, 1))

    def swap_sems(level):
        return swap_send.at[level], swap_recv.at[level]

    def result_start(level, total):
        result_near[level] = total
        send(
            result_near.at[level, 1 - core], result_far.at[level], swap_sems(level), partner
        )
        sends.append((result_far, 1, swap_sems(level)))
        out_ref[0, 0, mine, level_cols(level)] = result_near[level, core]

    def result_finish(level):
        wait_recv(result_far, 1, swap_sems(level))
        out_ref[0, 0, theirs, level_cols(level)] = result_far[level]

    group, wide = chips(1), nx
    corner = rank(1)

    def side(index):
        return side_send.at[index], side_recv.at[index]

    def turned(level):
        cols = slice(update_start(level), update_start(level + 1))
        straight, crossed = [], []
        for parity in range(2):
            high, low = split(update_raw[parity, :, cols].T)
            straight += [high, low]
            crossed += [low, high]
        return jnp.concatenate(
            [jnp.concatenate(straight, 1), jnp.concatenate(crossed, 1)], 0
        )

    def cross_start():
        picks = [chosen_columns(0, child, core) for child in range(2)]
        product = across(turned(1), jnp.concatenate(picks, 1))
        for block in range(group):
            for i in range(wide):
                cross_part[block, i] = product[
                    block * pivots : (block + 1) * pivots, i * pivots : (i + 1) * pivots
                ]
        for mask in far_first(group):
            send(
                cross_part.at[flip(corner, mask)],
                cross_landed.at[mask - 1],
                side(1),
                peer(1, mask),
            )
        sends.append((cross_landed, group - 1, side(1)))

    def cross_share():
        wait_recv(cross_landed, group - 1, side(1))
        total = cross_part[corner]
        for place in range(group - 1):
            total = total + cross_landed[place]
        span = cross_row.at[pl.ds(core * wide, wide)]
        cross_row[pl.ds(core * wide, wide)] = total
        send(span, span, side(2), partner)
        sends.append((cross_row, wide, side(2)))

    def cross_rows():
        wait_recv(cross_row, wide, side(2))
        for block in range(group):
            cols = slice(block * pivots, (block + 1) * pivots)
            high, low = split(cross_row[block])
            cross_row_split[:pivots, cols] = high
            cross_row_split[pivots:, cols] = low

    def cross_turn():
        for mask in far_first(group):
            send(cross_row.at[flip(corner, mask)], cross_col.at[corner], side(3), peer(1, mask))
        sends.append((cross_row, group - 1, side(3)))
        cross_col[corner] = cross_row[corner]

    def cross_columns():
        wait_recv(cross_col, group - 1, side(3))
        for block in range(group):
            high, low = split(cross_col[block])
            cross_col_split[block, :pivots] = high
            cross_col_split[block, pivots:] = low

    def low_start():
        left = turned(0)
        for target in range(nx):
            product = across(left, inverse_split[target * 2 + core])
            for i in range(nx):
                low_part[target, i] = product[i * pivots : (i + 1) * pivots]

    def low_spread():
        @on(1)
        def _():
            send(low_part.at[0], low_landed, side(4), peer(0, 1))

    def low_share():
        @on(0)
        def _():
            wait_recv(low_landed, nx, side(4))
            low_part[0] = low_part[0] + low_landed[...]

        low_sum[core] = low_part[column]
        send(low_sum.at[core], low_sum.at[core], side(5), partner)
        sends.append((low_landed, nx, side(5)))

    def low_finish():
        wait_recv(low_landed, nx, side(5))
        for i in range(nx):
            for parity in range(2):
                cols = slice(parity * pivots, (parity + 1) * pivots)
                high, low = split(low_sum[parity, i])
                low_split[i, :pivots, cols] = high
                low_split[i, pivots:, cols] = low

    def low_drain():
        @on(1)
        def _():
            wait_send(low_landed, nx, side(4))

    weighted = []
    one_across()
    two_beside()
    top_deep()
    prepare(0)
    prepare_update(0)
    base_ready()
    solved = fold(known_part(0))
    sent_up(solved, 0)
    one_beside()
    fetch_lists([0], True)
    two_across()
    prepare(1)
    prepare_update(1)
    cross_start()
    total = scatter_finish(("up", 0))
    gather_start(("up", 0), total)
    one_ready()
    known = known_part(1)
    sent_up(fold(known), 1)
    top_first()
    two_deep()
    fetch_lists(list(range(1, LEVELS - 1)), False)
    prepare(2)
    prepare_update(2)
    coefficient_copy.wait_recv()
    weighted.append(pivot_solve(solved, 0))
    low_start()
    gather_finish(("up", 0))
    cross_share()
    total = scatter_finish(("up", 1))
    cross_rows()
    values = [gathered["up", 0][block] for block in range(group)]
    total = total - fold(
        along_columns(rows_of(jnp.concatenate(values, 1)), cross_row_split[...])
    )
    gather_start(("up", 1), total)
    low_spread()
    solved = fold(less_children(known, 1))
    weighted.append(pivot_solve(solved, 1))
    top_second()
    two_ready()
    product = known_part(2)
    prepare(3)
    gather_finish(("up", 1))
    solved = fold(less_children(product, 2))
    sent_up(solved, 2)
    weighted.append(pivot_solve(solved, 2))
    low_share()
    total = scatter_finish(("up", 2))
    gather_start(("up", 2), total)
    cross_turn()
    sent_down(square_of(weighted[1]), 1)
    top_ready()
    product = known_part(3)
    low_finish()
    cross_columns()
    gather_finish(("up", 2))
    solved = fold(less_children(product, 3))
    weighted.append(pivot_solve(solved, 3))

    square = square_of(weighted[3])
    sent_down(square, 3)
    made_out(square, 3)
    final_first()
    made_out(square_of(weighted[0]), 0)
    plain_out_start(0)
    small = scatter_finish(("down", 0))
    total = scatter_finish(("down", 2))
    gather_start(("down", 2), total)
    final_second()
    gather_finish(("down", 2))
    square = square_of(with_parent(2))
    sent_down(square, 2)
    made_out(square, 2)
    middle_first()
    final_third()
    base = plain_out_finish(0)
    total = scatter_finish(("down", 1))
    gather_start(("down", 1), total)
    middle_second()
    gather_finish(("down", 1))
    for block in range(group):
        small = small - across(square_of(gathered["down", 1][block]), cross_col_split[block])
    gather_start(("down", 0), small)
    made_out(square_of(with_parent(1)), 1)
    plain_out_start(1)
    result_start(3, final_finish())
    middle_third()
    gather_finish(("down", 0))
    base = jnp.concatenate([base[0], base[1]], 1)
    for block in range(block_count(0)):
        base = base - across(square_of(gathered["down", 0][block]), low_split[block])
    result_start(0, jnp.stack([base[:, :pivots], base[:, pivots:]]))
    result_start(2, middle_finish())
    result_start(1, plain_out_finish(1))
    for level in (3, 0, 2, 1):
        result_finish(level)
    for item in sends:
        wait_send(*item)
    rhs_drain()
    for level in range(2):
        plain_out_drain(level)
    middle_drain()
    final_drain()
    low_drain()
    for copy in [*given.values(), *given_update.values(), coefficient_copy]:
        copy.wait_send()


def per_device(*arguments):
    right_side, factor_inverse, update_panel = arguments[:3]
    pivots = factor_inverse.shape[2]
    half = right_side.shape[2] // 2
    nx = lax.axis_size("front") // 2
    keys = [(kind, level) for kind in ("up", "down") for level in range(LEVELS - 1)]
    targets = (8, BLOCK)
    group, wide = nx << 1, nx
    blocks = factor_inverse.shape[3] // BLOCK
    buffers = []
    for _ in range(2):
        buffers += [pltpu.VMEM((nx << level, 2, half, pivots), F32) for level in range(LEVELS)]
    buffers += [pltpu.VMEM((nx << level, 2, half, pivots), F32) for level in range(LEVELS)]
    for kind, level in keys:
        wider, narrower = (nx << level + 1, nx << level)
        first, second = (wider, narrower) if kind == "up" else (narrower, wider)
        buffers += [pltpu.VMEM((count, half, BLOCK), F32) for count in (first, second, second)]
    vmem = pl.BlockSpec(memory_space=pltpu.VMEM)
    hbm = pl.BlockSpec(memory_space=pl.ANY)
    dma = pltpu.SemaphoreType.DMA
    square = (pivots, pivots)
    return pl.pallas_call(
        functools.partial(kernel, nx, pivots, keys),
        out_shape=pltpu.VMEM(right_side.shape, F32),
        in_specs=[vmem, hbm, hbm, vmem, vmem, vmem, vmem],
        out_specs=vmem,
        scratch_shapes=[
            pltpu.VMEM((2,) + factor_inverse.shape[2:], F32),
            pltpu.VMEM((2,) + update_panel.shape[2:], F32),
            pltpu.VMEM((blocks, 4 * pivots, BLOCK), BF16),
            pltpu.VMEM((4 * pivots, update_panel.shape[3]), BF16),
            pltpu.VMEM((2, 2, 8, LEVELS * pivots), F32),
            pltpu.VMEM(targets, jnp.int32),
            pltpu.VMEM((LEVELS - 1,) + targets, jnp.int32),
            pltpu.SMEM((LEVELS,) + targets, jnp.int32),
            pltpu.VMEM((LEVELS, 2, half, pivots), F32),
            pltpu.VMEM((LEVELS, half, pivots), F32),
            pltpu.VMEM((group, wide) + square, F32),
            pltpu.VMEM((group - 1, wide) + square, F32),
            pltpu.VMEM((group,) + square, F32),
            pltpu.VMEM((group,) + square, F32),
            pltpu.VMEM((2 * pivots, group * pivots), BF16),
            pltpu.VMEM((group, 2 * pivots, pivots), BF16),
            pltpu.VMEM((nx, nx) + square, F32),
            pltpu.VMEM((nx,) + square, F32),
            pltpu.VMEM((2, nx) + square, F32),
            pltpu.VMEM((nx, 2 * pivots, 2 * pivots), BF16),
            dma((2 * LEVELS + 1,)),
            dma((LEVELS - 1,)),
            dma((LEVELS - 1,)),
            dma((2 * LEVELS + 1,)),
            dma((2 * LEVELS + 1,)),
            dma((6,)),
            dma((6,)),
            dma((LEVELS, 4)),
            dma((LEVELS, 4)),
            dma((LEVELS, 3)),
            dma((LEVELS, 3)),
            dma((LEVELS,)),
            dma((LEVELS,)),
            dma((len(keys),)),
            dma((len(keys),)),
            dma((len(keys),)),
            dma((len(keys),)),
            *buffers,
        ],
        compiler_params=pltpu.CompilerParams(collective_id=0, has_side_effects=True),
    )(*arguments)


def solution(mesh):
    in_specs = (
        P("leaf", "front", None, None),
        P("leaf", "front", None, None),
        P("leaf", "front", None, None),
        P("leaf", None),
        P("leaf", "front", None),
        P("leaf", "front", None),
        P("leaf", "front", None),
    )
    out_specs = P("leaf", "front", None, None)
    return jax.shard_map(
        per_device, mesh=mesh, in_specs=in_specs, out_specs=out_specs, check_vma=False
    )
```

```python
import functools

import jax
import jax.numpy as jnp
from jax import lax
from jax.experimental import pallas as pl
from jax.experimental.pallas import tpu as pltpu
from jax.sharding import PartitionSpec as P

LEVELS = 4
BLOCK = 128
TOP = LEVELS - 1
DEPTH = 1 << TOP - 1
MESH = pl.DeviceIdType.MESH
F32 = jnp.float32
BF16 = jnp.bfloat16


def flip(value, mask):
    result = value
    bit = 0
    while mask >> bit:
        if mask >> bit & 1:
            unit = 1 << bit
            result = result + (1 - 2 * lax.rem(lax.div(value, unit), 2)) * unit
        bit += 1
    return result


def split(values):
    high = values.astype(BF16)
    return high, (values - high.astype(F32)).astype(BF16)


def rows_of(values):
    high, low = split(values)
    return jnp.concatenate([high, low], 0)


def square_of(values):
    rows = rows_of(values)
    pieces = []
    for start in range(0, rows.shape[1], BLOCK):
        pieces += [rows[:, start : start + BLOCK]] * 2
    return jnp.concatenate(pieces, 1)


def along_columns(stacked, matrix):
    return lax.dot_general(
        stacked, matrix, (((1,), (1,)), ((), ())), preferred_element_type=F32
    )


def fold(product):
    sides = product.shape[0] // 2
    both = product[:sides] + product[sides:]
    pieces = []
    for start in range(0, both.shape[1], 2 * BLOCK):
        pieces.append(
            both[:, start : start + BLOCK] + both[:, start + BLOCK : start + 2 * BLOCK]
        )
    return jnp.concatenate(pieces, 1)


def across(square, matrix):
    product = jnp.dot(square, matrix, preferred_element_type=F32)
    half = product.shape[0] // 2
    return product[:half] + product[half:]


def far_first(count):
    return sorted(range(1, count), key=lambda mask: (-(mask & DEPTH), -bin(mask).count("1")))


def kernel(nx, pivots, keys, *refs):
    (
        rhs_ref,
        inverse_hbm,
        update_hbm,
        lists_ref,
        pairs_ref,
        diagonal_ref,
        coupling_ref,
        out_ref,
        inverse_raw,
        update_raw,
        inverse_split,
        update_split,
        coefficients,
        targets_ref,
        targets_far,
        targets_smem,
        result_near,
        result_far,
        cross_part,
        cross_landed,
        cross_row,
        cross_col,
        cross_row_split,
        cross_col_split,
        low_part,
        low_landed,
        low_sum,
        low_split,
        load_sem,
        targets_send,
        targets_recv,
        weight_send,
        weight_recv,
        side_send,
        side_recv,
        rhs_send,
        rhs_recv,
        out_send,
        out_recv,
        swap_send,
        swap_recv,
        gather_send,
        gather_recv,
        scatter_send,
        scatter_recv,
        *buffers,
    ) = refs
    half = rhs_ref.shape[2] // 2
    leaf = lax.axis_index("leaf")
    front = lax.axis_index("front")
    core, column = lax.rem(front, 2), lax.div(front, 2)
    row = lax.rem(leaf, 2)
    buffers = list(buffers)
    rhs = [buffers.pop(0) for _ in range(LEVELS)]
    out_part = [buffers.pop(0) for _ in range(LEVELS)]
    out_landed = [buffers.pop(0) for _ in range(LEVELS)]
    gathered, part, landed = {}, {}, {}
    for key in keys:
        gathered[key] = buffers.pop(0)
        part[key] = buffers.pop(0)
        landed[key] = buffers.pop(0)

    def chips(level):
        return nx << level

    def rank(level):
        return column * (1 << level) + lax.rem(leaf, 1 << level)

    def peer(level, mask, other_core=False):
        near = 1 - core if other_core else core
        return flip(leaf, mask % (1 << level)), flip(column, (mask >> level) % nx) * 2 + near

    partner = (leaf, column * 2 + 1 - core)

    def slot_at(level, child, block):
        slot_column, offset = divmod(block, 1 << level)
        return (slot_column << level + 1) + (child << level) + offset

    def slot(level):
        inside = lax.rem(leaf, 1 << level)
        if level == TOP:
            return (row * nx + column) * DEPTH + lax.div(inside, 2)
        if level < 2:
            return rank(level)
        return lax.div(inside, 2) * (2 * nx) + column * 2 + row

    def slot_place(level, index):
        if level == TOP:
            rest, deep = divmod(index, DEPTH)
            slot_row, slot_column = divmod(rest, nx)
        elif level < 2:
            slot_column, offset = divmod(index, 1 << level)
            deep, slot_row = divmod(offset, 2)
        else:
            deep, rest = divmod(index, 2 * nx)
            slot_column, slot_row = divmod(rest, 2)
        return slot_column, deep * 2 + slot_row

    def slot_blocks(level, index):
        slot_column, offset = slot_place(level, index)
        first = column_start(level) // BLOCK
        return [first + ((slot_column * 2 + parity) << level) + offset for parity in range(2)]

    def column_start(level):
        return 2 * nx * pivots * ((1 << level) - 1)

    def update_start(level):
        return 2 * pivots * ((1 << level) - 1)

    def block_count(level):
        return 2 * pivots * (1 << level) // BLOCK

    sends = []

    def send(source, target, sems, device):
        pltpu.make_async_remote_copy(
            source, target, *sems, device_id=device, device_id_type=MESH
        ).start()

    def span_copy(buffer, count, sems):
        span = buffer.at[pl.ds(0, count)]
        return pltpu.make_async_remote_copy(
            span, span, *sems, device_id=partner, device_id_type=MESH
        )

    def wait_recv(buffer, count, sems):
        span_copy(buffer, count, sems).wait_recv()

    def wait_send(buffer, count, sems):
        span_copy(buffer, count, sems).wait_send()

    def on(slot_column, slot_core=None):
        if slot_core is None:
            return pl.when(column == slot_column)
        return pl.when((column == slot_column) & (core == slot_core))

    def for_column(body):
        for index in range(nx):

            @on(index)
            def _():
                body(index)

    loads = []
    for level in range(LEVELS):
        cols = pl.ds(column_start(level), column_start(level + 1) - column_start(level))
        loads.append(
            pltpu.make_async_copy(
                inverse_hbm.at[0, 0, :, cols], inverse_raw.at[core, :, cols], load_sem.at[level]
            )
        )
    loads.append(
        pltpu.make_async_copy(update_hbm.at[0, 0], update_raw.at[core], load_sem.at[LEVELS])
    )
    for index in (0, LEVELS, *range(1, LEVELS)):
        loads[index].start()

    mine = pl.ds(core * half, half)
    theirs = pl.ds((1 - core) * half, half)

    def level_cols(level):
        return slice(level * pivots, (level + 1) * pivots)

    for level in range(LEVELS):
        rhs[level][slot(level), core] = rhs_ref[0, 0, mine, level_cols(level)]

    @on(0)
    def _():
        zeros = jnp.zeros((2, half, pivots), F32)
        for level in range(1, LEVELS):
            for index in range(chips(level)):
                if slot_place(level, index)[0]:
                    rhs[level][index] = zeros

    @on(1)
    def _():
        zeros = jnp.zeros((2, half, pivots), F32)
        for level in range(2):
            for place in range((1 << level) - 1, chips(level) - 1):
                out_landed[level][place] = zeros
        for place in range(2):
            out_landed[2][2 * nx + place] = zeros

    targets_ref[...] = jnp.zeros_like(targets_ref)
    targets_ref[:1, : lists_ref.shape[1]] = lists_ref[...]

    def swap(values):
        width = values.shape[1]
        even = lax.rem(lax.broadcasted_iota(jnp.int32, values.shape, 1), 2) == 0
        return jnp.where(
            even, pltpu.roll(values, width - 1, 1), pltpu.roll(values, 1, 1)
        )

    def pivot_coefficients():
        width = diagonal_ref.shape[2]
        from_pair = (
            lax.div(lax.broadcasted_iota(jnp.int32, (width // 2, width), 1), 2)
            == lax.broadcasted_iota(jnp.int32, (width // 2, width), 0)
        ).astype(F32)
        pair_rows = jnp.concatenate(
            [
                jnp.broadcast_to(coupling_ref[0], (8, width // 2)),
                jnp.broadcast_to(pairs_ref[0].astype(F32), (8, width // 2)),
            ],
            0,
        )
        repeated = jnp.dot(
            pair_rows, from_pair, precision=lax.Precision.HIGHEST, preferred_element_type=F32
        )
        couple, flags = repeated[:8], repeated[8:] > 0.5
        diagonal = jnp.broadcast_to(diagonal_ref[0], (8, width))

        other_diagonal = swap(diagonal)
        determinant = diagonal * other_diagonal - couple * couple
        straight = jnp.where(flags, other_diagonal / determinant, 1.0 / diagonal)
        crossed = jnp.where(flags, -couple / determinant, 0.0)
        coefficients[core, 0] = straight
        coefficients[core, 1] = crossed

    def pivot_solve(solved, level):
        straight, crossed = [
            jnp.concatenate(
                [coefficients[parity, kind, :1, level_cols(level)] for parity in range(2)], 1
            )
            for kind in range(2)
        ]
        return solved * straight + swap(solved) * crossed

    barrier = pltpu.get_barrier_semaphore()
    everyone = [
        (flip(leaf, mask % (2 * DEPTH)), flip(front, mask // (2 * DEPTH)))
        for mask in range(1, 4 * nx * DEPTH)
    ]
    for device in everyone:
        pl.semaphore_signal(barrier, inc=1, device_id=device, device_id_type=MESH)
    pivot_coefficients()
    pl.semaphore_wait(barrier, len(everyone))

    def list_sems(level):
        return targets_send.at[level], targets_recv.at[level]

    def list_copy(level):
        return pltpu.make_async_remote_copy(
            targets_ref,
            targets_far.at[level],
            *list_sems(level),
            device_id=(flip(leaf, 1 << level), front),
            device_id_type=MESH,
        )

    def rhs_sems(level, phase):
        return rhs_send.at[level, phase], rhs_recv.at[level, phase]

    def weight_sems(index):
        return weight_send.at[index], weight_recv.at[index]

    def rhs_base():
        sems = rhs_sems(0, 0)
        target = rhs[0].at[column, core]
        source = rhs_ref.at[0, 0]
        for mask in range(1, nx):
            for each, there in ((mine, core), (theirs, 1 - core)):
                send(
                    source.at[each, pl.ds(0, pivots)],
                    target,
                    sems,
                    (leaf, flip(column, mask) * 2 + there),
                )
        send(source.at[theirs, pl.ds(0, pivots)], target, sems, partner)
        sends.append((rhs[0].at[0], 1, sems))
        sends.append((rhs[0], nx - 1, sems))

    def rhs_halves():
        for level in range(1, LEVELS):
            send(
                rhs_ref.at[0, 0, theirs, pl.ds(level * pivots, pivots)],
                rhs[level].at[slot(level), core],
                rhs_sems(level, 3),
                partner,
            )
            sends.append((rhs[level].at[0], 1, rhs_sems(level, 3)))

    def give_inverse(level):
        loads[level].wait()
        cols = pl.ds(column_start(level), column_start(level + 1) - column_start(level))
        span = inverse_raw.at[core, :, cols]
        copy = pltpu.make_async_remote_copy(
            span, span, *weight_sems(level), device_id=partner, device_id_type=MESH
        )
        copy.start()
        return copy

    def give_update(level):
        if not level:
            loads[LEVELS].wait()
        cols = pl.ds(update_start(level), update_start(level + 1) - update_start(level))
        span = update_raw.at[core, :, cols]
        copy = pltpu.make_async_remote_copy(
            span, span, *weight_sems(LEVELS + level), device_id=partner, device_id_type=MESH
        )
        copy.start()
        return copy

    list_copies = [list_copy(level) for level in range(LEVELS - 1)]
    rhs_base()
    for copy in list_copies:
        copy.start()
    rhs_halves()
    given, given_update = {}, {}
    given[0] = give_inverse(0)
    given_update[0] = give_update(0)
    given[1] = give_inverse(1)
    given_update[1] = give_update(1)
    coefficient_copy = pltpu.make_async_remote_copy(
        coefficients.at[core],
        coefficients.at[core],
        *weight_sems(2 * LEVELS),
        device_id=partner,
        device_id_type=MESH,
    )
    coefficient_copy.start()
    given[2] = give_inverse(2)
    given_update[2] = give_update(2)
    given[3] = give_inverse(3)

    def prepare(level):
        given[level].wait_recv()
        for block in range(column_start(level) // BLOCK, column_start(level + 1) // BLOCK):
            for parity in range(2):
                high, low = split(inverse_raw[parity, :, block * BLOCK : (block + 1) * BLOCK])
                start = parity * 2 * pivots
                inverse_split[block, start : start + pivots] = high
                inverse_split[block, start + pivots : start + 2 * pivots] = low

    def prepare_update(level):
        given_update[level].wait_recv()
        cols = slice(update_start(level), update_start(level + 1))
        for parity in range(2):
            high, low = split(update_raw[parity, :, cols])
            start = parity * 2 * pivots
            update_split[start : start + pivots, cols] = high
            update_split[start + pivots : start + 2 * pivots, cols] = low

    def fetch_lists(levels, own):
        for level in levels:
            list_copies[level].wait()
        lists = [(targets_ref, 0)] if own else []
        lists += [(targets_far.at[level], level + 1) for level in levels]
        copies = [
            pltpu.make_async_copy(source, targets_smem.at[index], load_sem.at[LEVELS + 1 + index])
            for source, index in lists
        ]
        for copy in copies:
            copy.start()
        for copy in copies:
            copy.wait()

    def half_ready(level):
        wait_recv(rhs[level].at[0], 1, rhs_sems(level, 3))

    def base_ready():
        wait_recv(rhs[0].reshape(nx * 2, half, pivots), 2 * nx - 1, rhs_sems(0, 0))

    def one_across():
        half_ready(1)

        @on(0)
        def _():
            each = rhs[1].at[rank(1)]
            send(each, each, rhs_sems(1, 0), peer(1, 2))

    def one_beside():
        def body(index):
            if index:
                wait_recv(rhs[1], index, rhs_sems(1, 0))
            for back in range(index + 1):
                each = rhs[1].at[rank(1) - 2 * back]
                send(each, each, rhs_sems(1, 1), peer(1, 1))

        for_column(body)

    def one_ready():
        for_column(lambda index: wait_recv(rhs[1], index + 1, rhs_sems(1, 1)))

    def pair_start():
        return lax.rem(lax.div(leaf, 2), 2) * (2 * nx)

    def two_beside():
        half_ready(2)
        each = rhs[2].at[slot(2)]
        send(each, each, rhs_sems(2, 1), peer(2, 1))
        sends.append((rhs[2], 1, rhs_sems(2, 1)))

    def two_across():
        wait_recv(rhs[2], 1, rhs_sems(2, 1))

        @on(0)
        def _():
            span = rhs[2].at[pl.ds(pair_start(), 2)]
            send(span, span, rhs_sems(2, 0), peer(2, 4))

    def two_deep():
        def body(index):
            if index:
                wait_recv(rhs[2], 2 * index, rhs_sems(2, 0))
            span = rhs[2].at[pl.ds(pair_start(), 2 * (index + 1))]
            send(span, span, rhs_sems(2, 2), peer(2, 2))

        for_column(body)

    def two_ready():
        for_column(lambda index: wait_recv(rhs[2], 2 * (index + 1), rhs_sems(2, 2)))

    def top_run(slot_row, slot_column):
        return rhs[TOP].at[pl.ds((slot_row * nx + slot_column) * DEPTH, DEPTH)]

    def top_deep():
        half_ready(TOP)
        each = rhs[TOP].at[slot(TOP)]
        for deep in range(DEPTH - 1, 0, -1):
            send(each, each, rhs_sems(TOP, 0), peer(TOP, 2 * deep))
        sends.append((rhs[TOP], DEPTH - 1, rhs_sems(TOP, 0)))

    def top_beside():
        run = top_run(row, column)
        send(run, run, rhs_sems(TOP, 2), peer(TOP, 1))

    def top_first():
        wait_recv(rhs[TOP], DEPTH - 1, rhs_sems(TOP, 0))

        @pl.when(core == 1)
        def _():
            top_beside()

        @on(0, 0)
        def _():
            run = top_run(row, 0)
            send(run, run, rhs_sems(TOP, 1), peer(TOP, 1 << TOP))

        sends.append((rhs[TOP], DEPTH, rhs_sems(TOP, 2)))

    def top_second():
        @pl.when(core == 0)
        def _():
            top_beside()

        @on(0, 1)
        def _():
            wait_recv(rhs[TOP], DEPTH, rhs_sems(TOP, 2))
            for each in range(2):
                run = top_run(each, 0)
                send(run, run, rhs_sems(TOP, 1), peer(TOP, 1 << TOP))

        @on(1, 0)
        def _():
            wait_recv(rhs[TOP], DEPTH, rhs_sems(TOP, 1))
            run = top_run(row, 0)
            send(run, run, rhs_sems(TOP, 2), peer(TOP, 1))

    def top_ready():
        @on(0, 0)
        def _():
            wait_recv(rhs[TOP], DEPTH, rhs_sems(TOP, 2))

        @on(1, 0)
        def _():
            wait_recv(rhs[TOP], 2 * DEPTH, rhs_sems(TOP, 2))

        @on(1, 1)
        def _():
            wait_recv(rhs[TOP], DEPTH, rhs_sems(TOP, 2))
            wait_recv(rhs[TOP], 2 * DEPTH, rhs_sems(TOP, 1))

    def rhs_drain():
        def body(index):
            if not index:
                wait_send(rhs[1], 1, rhs_sems(1, 0))
                wait_send(rhs[2], 2, rhs_sems(2, 0))
            wait_send(rhs[1], index + 1, rhs_sems(1, 1))
            wait_send(rhs[2], 2 * (index + 1), rhs_sems(2, 2))

        for_column(body)

        @on(0, 0)
        def _():
            wait_send(rhs[TOP], DEPTH, rhs_sems(TOP, 1))

        @on(0, 1)
        def _():
            wait_send(rhs[TOP], 2 * DEPTH, rhs_sems(TOP, 1))

        @on(1, 0)
        def _():
            wait_send(rhs[TOP], DEPTH, rhs_sems(TOP, 2))

    def group_of(key):
        return key[1] + (1 if key[0] == "up" else 0), key[1] + (0 if key[0] == "up" else 1)

    def key_sems(kind, key):
        index = keys.index(key)
        if kind == "gather":
            return gather_send.at[index], gather_recv.at[index]
        return scatter_send.at[index], scatter_recv.at[index]

    def gather_start(key, total):
        level, _ = group_of(key)
        buffer, sems = gathered[key], key_sems("gather", key)
        buffer[rank(level)] = total
        for mask in far_first(chips(level)):
            each = buffer.at[rank(level)]
            send(each, each, sems, peer(level, mask))
        sends.append((buffer, chips(level) - 1, sems))

    def gather_finish(key):
        level, _ = group_of(key)
        wait_recv(gathered[key], chips(level) - 1, key_sems("gather", key))

    def scatter_start(key):
        _, level = group_of(key)
        sems = key_sems("scatter", key)
        for mask in far_first(chips(level)):
            send(
                part[key].at[flip(rank(level), mask)],
                landed[key].at[mask - 1],
                sems,
                peer(level, mask),
            )
        sends.append((part[key], chips(level) - 1, sems))

    def scatter_finish(key):
        _, level = group_of(key)
        wait_recv(landed[key], chips(level) - 1, key_sems("scatter", key))
        total = part[key][rank(level)]
        for place in range(chips(level) - 1):
            total = total + landed[key][place]
        return total

    def chosen_columns(level, child, index):
        place = update_start(level) // BLOCK + index
        upper = lax.rem(lax.div(leaf, 1 << level), 2)
        near, far = targets_smem[0, 0, place], targets_smem[level + 1, 0, place]
        block = near + (far - near) * (upper + child - 2 * upper * child)
        return inverse_split[column_start(level + 1) // BLOCK + block]

    def known_part(level):
        product = None
        for index in range(chips(level)):
            values = jnp.concatenate([rhs[level][index, parity] for parity in range(2)], 1)
            matrix = jnp.concatenate(
                [inverse_split[block] for block in slot_blocks(level, index)], 1
            )
            term = along_columns(rows_of(values), matrix)
            product = term if product is None else product + term
        return product

    def sent_up(solved, level):
        start, blocks = update_start(level), block_count(level)
        partial = across(square_of(solved), update_split[:, start : start + blocks * BLOCK])
        for block in range(blocks):
            part["up", level][block] = partial[:, block * BLOCK : (block + 1) * BLOCK]
        scatter_start(("up", level))

    def less_children(product, level):
        below = level - 1
        buffer = gathered["up", below]
        for child in range(2):
            for index in range(0, block_count(below), 2):
                pair = (index, index + 1)
                values = [buffer[slot_at(below, child, i)] for i in pair]
                matrices = [chosen_columns(below, child, i) for i in pair]
                product = product - along_columns(
                    rows_of(jnp.concatenate(values, 1)), jnp.concatenate(matrices, 1)
                )
        return product

    def sent_down(square, level):
        key = ("down", level - 1)
        for child in range(2):
            for index in range(0, block_count(level - 1), 2):
                pair = (index, index + 1)
                matrix = jnp.concatenate(
                    [chosen_columns(level - 1, child, i) for i in pair], 1
                )
                partial = across(square, matrix)
                for j, i in enumerate(pair):
                    part[key][slot_at(level - 1, child, i)] = partial[
                        :, j * BLOCK : (j + 1) * BLOCK
                    ]
        scatter_start(key)

    def with_parent(level):
        buffer = gathered["down", level]
        product = None
        for index in range(0, block_count(level), 2):
            values = jnp.concatenate([buffer[index], buffer[index + 1]], 1)
            start = update_start(level) + index * BLOCK
            term = along_columns(rows_of(values), update_split[:, start : start + 2 * BLOCK])
            product = term if product is None else product + term
        return weighted[level] - fold(product)

    def out_sems(level, phase):
        return out_send.at[level, phase], out_recv.at[level, phase]

    def made_out(square, level):
        for index in range(chips(level)):
            matrix = jnp.concatenate(
                [inverse_split[block] for block in slot_blocks(level, index)], 1
            )
            partial = across(square, matrix)
            for parity in range(2):
                out_part[level][index, parity] = partial[
                    :, parity * pivots : (parity + 1) * pivots
                ]

    def plain_out_start(level):
        sems = out_sems(level, 0)

        def one(mask):
            send(
                out_part[level].at[flip(rank(level), mask)],
                out_landed[level].at[mask - 1],
                sems,
                peer(level, mask),
            )

        @on(1)
        def _():
            for mask in far_first(chips(level)):
                if mask >> level:
                    one(mask)

        for mask in far_first(1 << level):
            one(mask)

    def plain_out_finish(level):
        def body(index):
            fewer = chips(level) if index == 0 else 1 << level
            if fewer > 1:
                wait_recv(out_landed[level], fewer - 1, out_sems(level, 0))

        for_column(body)
        total = out_part[level][rank(level)]
        for place in range(chips(level) - 1):
            total = total + out_landed[level][place]
        return total

    def plain_out_drain(level):
        def body(index):
            fewer = chips(level) if index else 1 << level
            if fewer > 1:
                wait_send(out_landed[level], fewer - 1, out_sems(level, 0))

        for_column(body)

    def out_add(level, start, place, count):
        span = pl.ds(start, count)
        out_part[level][span] = out_part[level][span] + out_landed[level][place : place + count]

    def middle_first():
        other = (1 - lax.rem(lax.div(leaf, 2), 2)) * (2 * nx)

        def body(index):
            each = 2 * (index + 1)
            send(
                out_part[2].at[pl.ds(other, each)],
                out_landed[2].at[pl.ds(0, each)],
                out_sems(2, 0),
                peer(2, 2),
            )

        for_column(body)

    def middle_second():
        here = pair_start() + row
        beside = pair_start() + 1 - row

        def body(index):
            each = 2 * (index + 1)
            wait_recv(out_landed[2], each, out_sems(2, 0))
            out_add(2, pair_start(), 0, each)
            if index:
                for place, source, mask in ((1, beside, 5), (0, here, 4)):
                    send(
                        out_part[2].at[source],
                        out_landed[2].at[2 * nx + place],
                        out_sems(2, 1),
                        peer(2, mask),
                    )
            send(
                out_part[2].at[beside + 2 * index],
                out_landed[2].at[2 * nx + 2],
                out_sems(2, 1),
                peer(2, 1),
            )

        for_column(body)

    def middle_finish():
        def body(index):
            wait_recv(out_landed[2], 1 if index else nx + 1, out_sems(2, 1))

        for_column(body)
        total = out_part[2][slot(2)]
        for place in range(3):
            total = total + out_landed[2][2 * nx + place]
        return total

    def middle_drain():
        def body(index):
            wait_send(out_landed[2], 2 * (index + 1), out_sems(2, 0))
            wait_send(out_landed[2], nx + 1 if index else 1, out_sems(2, 1))

        for_column(body)

    def final_index(slot_row, slot_column):
        return (slot_row * nx + slot_column) * DEPTH

    def final_run(slot_row, slot_column, count=1):
        return out_part[TOP].at[pl.ds(final_index(slot_row, slot_column), count * DEPTH)]

    def final_first():
        for index in range(nx):

            @on(index, 0)
            def _():
                send(
                    final_run(1 - row, 0, index + 1),
                    out_landed[TOP].at[pl.ds(0, (index + 1) * DEPTH)],
                    out_sems(TOP, 0),
                    peer(TOP, 1),
                )

        @on(1, 1)
        def _():
            for each in range(2):
                send(
                    final_run(each, 0),
                    out_landed[TOP].at[pl.ds(each * DEPTH, DEPTH)],
                    out_sems(TOP, 0),
                    peer(TOP, 1 << TOP),
                )

    def final_second():
        there = out_landed[TOP].at[pl.ds(2 * DEPTH, DEPTH)]
        for index in range(nx):

            @on(index, 0)
            def _():
                wait_recv(out_landed[TOP], (index + 1) * DEPTH, out_sems(TOP, 0))
                out_add(TOP, final_index(row, 0), 0, (index + 1) * DEPTH)

        @on(1, 0)
        def _():
            send(final_run(row, 0), there, out_sems(TOP, 1), peer(TOP, 1 << TOP))

        @on(0, 1)
        def _():
            wait_recv(out_landed[TOP], 2 * DEPTH, out_sems(TOP, 0))
            for each in range(2):
                out_add(TOP, final_index(each, 0), each * DEPTH, DEPTH)

        @pl.when(core == 1)
        def _():
            send(final_run(1 - row, column), there, out_sems(TOP, 1), peer(TOP, 1))

    def final_third():
        @pl.when((core == 1) | (column == 0))
        def _():
            wait_recv(out_landed[TOP], DEPTH, out_sems(TOP, 1))
            out_add(TOP, final_index(row, column), 2 * DEPTH, DEPTH)

        deep = lax.rem(lax.div(leaf, 2), DEPTH)
        for mask in range(DEPTH - 1, 0, -1):
            send(
                out_part[TOP].at[final_index(row, column) + flip(deep, mask)],
                out_landed[TOP].at[3 * DEPTH + mask - 1],
                out_sems(TOP, 2),
                peer(TOP, 2 * mask),
            )
        sends.append((out_landed[TOP], DEPTH - 1, out_sems(TOP, 2)))

    def final_finish():
        wait_recv(out_landed[TOP], DEPTH - 1, out_sems(TOP, 2))
        total = out_part[TOP][slot(TOP)]
        for place in range(DEPTH - 1):
            total = total + out_landed[TOP][3 * DEPTH + place]
        return total

    def final_drain():
        for index in range(nx):

            @on(index, 0)
            def _():
                wait_send(out_landed[TOP], (index + 1) * DEPTH, out_sems(TOP, 0))

        @on(1, 1)
        def _():
            wait_send(out_landed[TOP], 2 * DEPTH, out_sems(TOP, 0))

        @pl.when((core == 1) | (column == 1))
        def _():
            wait_send(out_landed[TOP], DEPTH, out_sems(TOP, 1))

    def swap_sems(level):
        return swap_send.at[level], swap_recv.at[level]

    def result_start(level, total):
        result_near[level] = total
        send(
            result_near.at[level, 1 - core], result_far.at[level], swap_sems(level), partner
        )
        sends.append((result_far, 1, swap_sems(level)))
        out_ref[0, 0, mine, level_cols(level)] = result_near[level, core]

    def result_finish(level):
        wait_recv(result_far, 1, swap_sems(level))
        out_ref[0, 0, theirs, level_cols(level)] = result_far[level]

    group, wide = chips(1), nx
    corner = rank(1)

    def side(index):
        return side_send.at[index], side_recv.at[index]

    def turned(level):
        cols = slice(update_start(level), update_start(level + 1))
        straight, crossed = [], []
        for parity in range(2):
            high, low = split(update_raw[parity, :, cols].T)
            straight += [high, low]
            crossed += [low, high]
        return jnp.concatenate(
            [jnp.concatenate(straight, 1), jnp.concatenate(crossed, 1)], 0
        )

    def cross_start():
        picks = [chosen_columns(0, child, core) for child in range(2)]
        product = across(turned(1), jnp.concatenate(picks, 1))
        for block in range(group):
            for i in range(wide):
                cross_part[block, i] = product[
                    block * pivots : (block + 1) * pivots, i * pivots : (i + 1) * pivots
                ]
        for mask in far_first(group):
            send(
                cross_part.at[flip(corner, mask)],
                cross_landed.at[mask - 1],
                side(1),
                peer(1, mask),
            )
        sends.append((cross_landed, group - 1, side(1)))

    def cross_share():
        wait_recv(cross_landed, group - 1, side(1))
        total = cross_part[corner]
        for place in range(group - 1):
            total = total + cross_landed[place]
        span = cross_row.at[pl.ds(core * wide, wide)]
        cross_row[pl.ds(core * wide, wide)] = total
        send(span, span, side(2), partner)
        sends.append((cross_row, wide, side(2)))

    def cross_rows():
        wait_recv(cross_row, wide, side(2))
        for block in range(group):
            cols = slice(block * pivots, (block + 1) * pivots)
            high, low = split(cross_row[block])
            cross_row_split[:pivots, cols] = high
            cross_row_split[pivots:, cols] = low

    def cross_turn():
        for mask in far_first(group):
            send(cross_row.at[flip(corner, mask)], cross_col.at[corner], side(3), peer(1, mask))
        sends.append((cross_row, group - 1, side(3)))
        cross_col[corner] = cross_row[corner]

    def cross_columns():
        wait_recv(cross_col, group - 1, side(3))
        for block in range(group):
            high, low = split(cross_col[block])
            cross_col_split[block, :pivots] = high
            cross_col_split[block, pivots:] = low

    def low_start():
        left = turned(0)
        for target in range(nx):
            product = across(left, inverse_split[target * 2 + core])
            for i in range(nx):
                low_part[target, i] = product[i * pivots : (i + 1) * pivots]

    def low_spread():
        @on(1)
        def _():
            send(low_part.at[0], low_landed, side(4), peer(0, 1))

    def low_share():
        @on(0)
        def _():
            wait_recv(low_landed, nx, side(4))
            low_part[0] = low_part[0] + low_landed[...]

        low_sum[core] = low_part[column]
        send(low_sum.at[core], low_sum.at[core], side(5), partner)
        sends.append((low_landed, nx, side(5)))

    def low_finish():
        wait_recv(low_landed, nx, side(5))
        for i in range(nx):
            for parity in range(2):
                cols = slice(parity * pivots, (parity + 1) * pivots)
                high, low = split(low_sum[parity, i])
                low_split[i, :pivots, cols] = high
                low_split[i, pivots:, cols] = low

    def low_drain():
        @on(1)
        def _():
            wait_send(low_landed, nx, side(4))

    weighted = []
    one_across()
    two_beside()
    top_deep()
    prepare(0)
    prepare_update(0)
    base_ready()
    solved = fold(known_part(0))
    sent_up(solved, 0)
    one_beside()
    fetch_lists([0], True)
    two_across()
    prepare(1)
    prepare_update(1)
    cross_start()
    total = scatter_finish(("up", 0))
    gather_start(("up", 0), total)
    one_ready()
    known = known_part(1)
    sent_up(fold(known), 1)
    top_first()
    two_deep()
    fetch_lists(list(range(1, LEVELS - 1)), False)
    prepare(2)
    prepare_update(2)
    coefficient_copy.wait_recv()
    weighted.append(pivot_solve(solved, 0))
    low_start()
    gather_finish(("up", 0))
    cross_share()
    total = scatter_finish(("up", 1))
    cross_rows()
    values = [gathered["up", 0][block] for block in range(group)]
    total = total - fold(
        along_columns(rows_of(jnp.concatenate(values, 1)), cross_row_split[...])
    )
    gather_start(("up", 1), total)
    low_spread()
    solved = fold(less_children(known, 1))
    weighted.append(pivot_solve(solved, 1))
    top_second()
    two_ready()
    product = known_part(2)
    prepare(3)
    gather_finish(("up", 1))
    solved = fold(less_children(product, 2))
    sent_up(solved, 2)
    weighted.append(pivot_solve(solved, 2))
    low_share()
    total = scatter_finish(("up", 2))
    gather_start(("up", 2), total)
    cross_turn()
    sent_down(square_of(weighted[1]), 1)
    top_ready()
    product = known_part(3)
    low_finish()
    gather_finish(("up", 2))
    solved = fold(less_children(product, 3))
    weighted.append(pivot_solve(solved, 3))

    square = square_of(weighted[3])
    sent_down(square, 3)
    made_out(square, 3)
    final_first()
    made_out(square_of(weighted[0]), 0)
    plain_out_start(0)
    cross_columns()
    small = scatter_finish(("down", 0))
    total = scatter_finish(("down", 2))
    gather_start(("down", 2), total)
    final_second()
    gather_finish(("down", 2))
    square = square_of(with_parent(2))
    sent_down(square, 2)
    made_out(square, 2)
    middle_first()
    final_third()
    base = plain_out_finish(0)
    total = scatter_finish(("down", 1))
    gather_start(("down", 1), total)
    middle_second()
    gather_finish(("down", 1))
    made_out(square_of(with_parent(1)), 1)
    plain_out_start(1)
    for block in range(group):
        small = small - across(square_of(gathered["down", 1][block]), cross_col_split[block])
    gather_start(("down", 0), small)
    result_start(3, final_finish())
    gather_finish(("down", 0))
    base = jnp.concatenate([base[0], base[1]], 1)
    for block in range(block_count(0)):
        base = base - across(square_of(gathered["down", 0][block]), low_split[block])
    result_start(0, jnp.stack([base[:, :pivots], base[:, pivots:]]))
    result_start(2, middle_finish())
    result_start(1, plain_out_finish(1))
    for level in (3, 0, 2, 1):
        result_finish(level)
    for item in sends:
        wait_send(*item)
    rhs_drain()
    for level in range(2):
        plain_out_drain(level)
    middle_drain()
    final_drain()
    low_drain()
    for copy in [*given.values(), *given_update.values(), coefficient_copy]:
        copy.wait_send()


def per_device(*arguments):
    right_side, factor_inverse, update_panel = arguments[:3]
    pivots = factor_inverse.shape[2]
    half = right_side.shape[2] // 2
    nx = lax.axis_size("front") // 2
    keys = [(kind, level) for kind in ("up", "down") for level in range(LEVELS - 1)]
    targets = (8, BLOCK)
    group, wide = nx << 1, nx
    blocks = factor_inverse.shape[3] // BLOCK
    buffers = []
    for _ in range(2):
        buffers += [pltpu.VMEM((nx << level, 2, half, pivots), F32) for level in range(LEVELS)]
    buffers += [pltpu.VMEM((nx << level, 2, half, pivots), F32) for level in range(LEVELS)]
    for kind, level in keys:
        wider, narrower = (nx << level + 1, nx << level)
        first, second = (wider, narrower) if kind == "up" else (narrower, wider)
        buffers += [pltpu.VMEM((count, half, BLOCK), F32) for count in (first, second, second)]
    vmem = pl.BlockSpec(memory_space=pltpu.VMEM)
    hbm = pl.BlockSpec(memory_space=pl.ANY)
    dma = pltpu.SemaphoreType.DMA
    square = (pivots, pivots)
    return pl.pallas_call(
        functools.partial(kernel, nx, pivots, keys),
        out_shape=pltpu.VMEM(right_side.shape, F32),
        in_specs=[vmem, hbm, hbm, vmem, vmem, vmem, vmem],
        out_specs=vmem,
        scratch_shapes=[
            pltpu.VMEM((2,) + factor_inverse.shape[2:], F32),
            pltpu.VMEM((2,) + update_panel.shape[2:], F32),
            pltpu.VMEM((blocks, 4 * pivots, BLOCK), BF16),
            pltpu.VMEM((4 * pivots, update_panel.shape[3]), BF16),
            pltpu.VMEM((2, 2, 8, LEVELS * pivots), F32),
            pltpu.VMEM(targets, jnp.int32),
            pltpu.VMEM((LEVELS - 1,) + targets, jnp.int32),
            pltpu.SMEM((LEVELS,) + targets, jnp.int32),
            pltpu.VMEM((LEVELS, 2, half, pivots), F32),
            pltpu.VMEM((LEVELS, half, pivots), F32),
            pltpu.VMEM((group, wide) + square, F32),
            pltpu.VMEM((group - 1, wide) + square, F32),
            pltpu.VMEM((group,) + square, F32),
            pltpu.VMEM((group,) + square, F32),
            pltpu.VMEM((2 * pivots, group * pivots), BF16),
            pltpu.VMEM((group, 2 * pivots, pivots), BF16),
            pltpu.VMEM((nx, nx) + square, F32),
            pltpu.VMEM((nx,) + square, F32),
            pltpu.VMEM((2, nx) + square, F32),
            pltpu.VMEM((nx, 2 * pivots, 2 * pivots), BF16),
            dma((2 * LEVELS + 1,)),
            dma((LEVELS - 1,)),
            dma((LEVELS - 1,)),
            dma((2 * LEVELS + 1,)),
            dma((2 * LEVELS + 1,)),
            dma((6,)),
            dma((6,)),
            dma((LEVELS, 4)),
            dma((LEVELS, 4)),
            dma((LEVELS, 3)),
            dma((LEVELS, 3)),
            dma((LEVELS,)),
            dma((LEVELS,)),
            dma((len(keys),)),
            dma((len(keys),)),
            dma((len(keys),)),
            dma((len(keys),)),
            *buffers,
        ],
        compiler_params=pltpu.CompilerParams(collective_id=0, has_side_effects=True),
    )(*arguments)


def solution(mesh):
    in_specs = (
        P("leaf", "front", None, None),
        P("leaf", "front", None, None),
        P("leaf", "front", None, None),
        P("leaf", None),
        P("leaf", "front", None),
        P("leaf", "front", None),
        P("leaf", "front", None),
    )
    out_specs = P("leaf", "front", None, None)
    return jax.shard_map(
        per_device, mesh=mesh, in_specs=in_specs, out_specs=out_specs, check_vma=False
    )
```

```python
import functools

import jax
import jax.numpy as jnp
from jax import lax
from jax.experimental import pallas as pl
from jax.experimental.pallas import tpu as pltpu
from jax.sharding import PartitionSpec as P

LEVELS = 4
BLOCK = 128
TOP = LEVELS - 1
DEPTH = 1 << TOP - 1
MESH = pl.DeviceIdType.MESH
F32 = jnp.float32
BF16 = jnp.bfloat16


def flip(value, mask):
    result = value
    bit = 0
    while mask >> bit:
        if mask >> bit & 1:
            unit = 1 << bit
            result = result + (1 - 2 * lax.rem(lax.div(value, unit), 2)) * unit
        bit += 1
    return result


def split(values):
    high = values.astype(BF16)
    return high, (values - high.astype(F32)).astype(BF16)


def rows_of(values):
    high, low = split(values)
    return jnp.concatenate([high, low], 0)


def square_of(values):
    rows = rows_of(values)
    pieces = []
    for start in range(0, rows.shape[1], BLOCK):
        pieces += [rows[:, start : start + BLOCK]] * 2
    return jnp.concatenate(pieces, 1)


def along_columns(stacked, matrix):
    return lax.dot_general(
        stacked, matrix, (((1,), (1,)), ((), ())), preferred_element_type=F32
    )


def fold(product):
    sides = product.shape[0] // 2
    both = product[:sides] + product[sides:]
    pieces = []
    for start in range(0, both.shape[1], 2 * BLOCK):
        pieces.append(
            both[:, start : start + BLOCK] + both[:, start + BLOCK : start + 2 * BLOCK]
        )
    return jnp.concatenate(pieces, 1)


def across(square, matrix):
    product = jnp.dot(square, matrix, preferred_element_type=F32)
    half = product.shape[0] // 2
    return product[:half] + product[half:]


def far_first(count):
    return sorted(range(1, count), key=lambda mask: (-(mask & DEPTH), -bin(mask).count("1")))


def kernel(nx, pivots, keys, *refs):
    (
        rhs_ref,
        inverse_hbm,
        update_hbm,
        lists_ref,
        pairs_ref,
        diagonal_ref,
        coupling_ref,
        out_ref,
        inverse_raw,
        update_raw,
        inverse_split,
        update_split,
        coefficients,
        targets_ref,
        targets_far,
        targets_smem,
        result_near,
        result_far,
        cross_part,
        cross_landed,
        cross_row,
        cross_col,
        cross_row_split,
        cross_col_split,
        low_part,
        low_landed,
        low_sum,
        low_split,
        load_sem,
        targets_send,
        targets_recv,
        weight_send,
        weight_recv,
        side_send,
        side_recv,
        rhs_send,
        rhs_recv,
        out_send,
        out_recv,
        swap_send,
        swap_recv,
        gather_send,
        gather_recv,
        scatter_send,
        scatter_recv,
        *buffers,
    ) = refs
    half = rhs_ref.shape[2] // 2
    leaf = lax.axis_index("leaf")
    front = lax.axis_index("front")
    core, column = lax.rem(front, 2), lax.div(front, 2)
    row = lax.rem(leaf, 2)
    buffers = list(buffers)
    rhs = [buffers.pop(0) for _ in range(LEVELS)]
    out_part = [buffers.pop(0) for _ in range(LEVELS)]
    out_landed = [buffers.pop(0) for _ in range(LEVELS)]
    gathered, part, landed = {}, {}, {}
    for key in keys:
        gathered[key] = buffers.pop(0)
        part[key] = buffers.pop(0)
        landed[key] = buffers.pop(0)

    def chips(level):
        return nx << level

    def rank(level):
        return column * (1 << level) + lax.rem(leaf, 1 << level)

    def peer(level, mask, other_core=False):
        near = 1 - core if other_core else core
        return flip(leaf, mask % (1 << level)), flip(column, (mask >> level) % nx) * 2 + near

    partner = (leaf, column * 2 + 1 - core)

    def slot_at(level, child, block):
        slot_column, offset = divmod(block, 1 << level)
        return (slot_column << level + 1) + (child << level) + offset

    def slot(level):
        inside = lax.rem(leaf, 1 << level)
        if level == TOP:
            return (row * nx + column) * DEPTH + lax.div(inside, 2)
        if level < 2:
            return rank(level)
        return lax.div(inside, 2) * (2 * nx) + column * 2 + row

    def slot_place(level, index):
        if level == TOP:
            rest, deep = divmod(index, DEPTH)
            slot_row, slot_column = divmod(rest, nx)
        elif level < 2:
            slot_column, offset = divmod(index, 1 << level)
            deep, slot_row = divmod(offset, 2)
        else:
            deep, rest = divmod(index, 2 * nx)
            slot_column, slot_row = divmod(rest, 2)
        return slot_column, deep * 2 + slot_row

    def slot_blocks(level, index):
        slot_column, offset = slot_place(level, index)
        first = column_start(level) // BLOCK
        return [first + ((slot_column * 2 + parity) << level) + offset for parity in range(2)]

    def column_start(level):
        return 2 * nx * pivots * ((1 << level) - 1)

    def update_start(level):
        return 2 * pivots * ((1 << level) - 1)

    def block_count(level):
        return 2 * pivots * (1 << level) // BLOCK

    sends = []

    def send(source, target, sems, device):
        pltpu.make_async_remote_copy(
            source, target, *sems, device_id=device, device_id_type=MESH
        ).start()

    def span_copy(buffer, count, sems):
        span = buffer.at[pl.ds(0, count)]
        return pltpu.make_async_remote_copy(
            span, span, *sems, device_id=partner, device_id_type=MESH
        )

    def wait_recv(buffer, count, sems):
        span_copy(buffer, count, sems).wait_recv()

    def wait_send(buffer, count, sems):
        span_copy(buffer, count, sems).wait_send()

    def on(slot_column, slot_core=None):
        if slot_core is None:
            return pl.when(column == slot_column)
        return pl.when((column == slot_column) & (core == slot_core))

    def for_column(body):
        for index in range(nx):

            @on(index)
            def _():
                body(index)

    loads = []
    for level in range(LEVELS):
        cols = pl.ds(column_start(level), column_start(level + 1) - column_start(level))
        loads.append(
            pltpu.make_async_copy(
                inverse_hbm.at[0, 0, :, cols], inverse_raw.at[core, :, cols], load_sem.at[level]
            )
        )
    loads.append(
        pltpu.make_async_copy(update_hbm.at[0, 0], update_raw.at[core], load_sem.at[LEVELS])
    )
    for index in (0, LEVELS, *range(1, LEVELS)):
        loads[index].start()

    mine = pl.ds(core * half, half)
    theirs = pl.ds((1 - core) * half, half)

    def level_cols(level):
        return slice(level * pivots, (level + 1) * pivots)

    for level in range(LEVELS):
        rhs[level][slot(level), core] = rhs_ref[0, 0, mine, level_cols(level)]

    @on(0)
    def _():
        zeros = jnp.zeros((2, half, pivots), F32)
        for level in range(1, LEVELS):
            for index in range(chips(level)):
                if slot_place(level, index)[0]:
                    rhs[level][index] = zeros

    @on(1)
    def _():
        zeros = jnp.zeros((2, half, pivots), F32)
        for level in range(2):
            for place in range((1 << level) - 1, chips(level) - 1):
                out_landed[level][place] = zeros
        for place in range(2):
            out_landed[2][2 * nx + place] = zeros

    targets_ref[...] = jnp.zeros_like(targets_ref)
    targets_ref[:1, : lists_ref.shape[1]] = lists_ref[...]

    def swap(values):
        width = values.shape[1]
        even = lax.rem(lax.broadcasted_iota(jnp.int32, values.shape, 1), 2) == 0
        return jnp.where(
            even, pltpu.roll(values, width - 1, 1), pltpu.roll(values, 1, 1)
        )

    def pivot_coefficients():
        width = diagonal_ref.shape[2]
        from_pair = (
            lax.div(lax.broadcasted_iota(jnp.int32, (width // 2, width), 1), 2)
            == lax.broadcasted_iota(jnp.int32, (width // 2, width), 0)
        ).astype(F32)
        pair_rows = jnp.concatenate(
            [
                jnp.broadcast_to(coupling_ref[0], (8, width // 2)),
                jnp.broadcast_to(pairs_ref[0].astype(F32), (8, width // 2)),
            ],
            0,
        )
        repeated = jnp.dot(
            pair_rows, from_pair, precision=lax.Precision.HIGHEST, preferred_element_type=F32
        )
        couple, flags = repeated[:8], repeated[8:] > 0.5
        diagonal = jnp.broadcast_to(diagonal_ref[0], (8, width))

        other_diagonal = swap(diagonal)
        determinant = diagonal * other_diagonal - couple * couple
        straight = jnp.where(flags, other_diagonal / determinant, 1.0 / diagonal)
        crossed = jnp.where(flags, -couple / determinant, 0.0)
        coefficients[core, 0] = straight
        coefficients[core, 1] = crossed

    def pivot_solve(solved, level):
        straight, crossed = [
            jnp.concatenate(
                [coefficients[parity, kind, :1, level_cols(level)] for parity in range(2)], 1
            )
            for kind in range(2)
        ]
        return solved * straight + swap(solved) * crossed

    barrier = pltpu.get_barrier_semaphore()
    everyone = [
        (flip(leaf, mask % (2 * DEPTH)), flip(front, mask // (2 * DEPTH)))
        for mask in range(1, 4 * nx * DEPTH)
    ]
    for device in everyone:
        pl.semaphore_signal(barrier, inc=1, device_id=device, device_id_type=MESH)
    pl.semaphore_wait(barrier, len(everyone))

    def list_sems(level):
        return targets_send.at[level], targets_recv.at[level]

    def list_copy(level):
        return pltpu.make_async_remote_copy(
            targets_ref,
            targets_far.at[level],
            *list_sems(level),
            device_id=(flip(leaf, 1 << level), front),
            device_id_type=MESH,
        )

    def rhs_sems(level, phase):
        return rhs_send.at[level, phase], rhs_recv.at[level, phase]

    def weight_sems(index):
        return weight_send.at[index], weight_recv.at[index]

    def rhs_base():
        sems = rhs_sems(0, 0)
        target = rhs[0].at[column, core]
        source = rhs_ref.at[0, 0]
        for mask in range(1, nx):
            for each, there in ((mine, core), (theirs, 1 - core)):
                send(
                    source.at[each, pl.ds(0, pivots)],
                    target,
                    sems,
                    (leaf, flip(column, mask) * 2 + there),
                )
        send(source.at[theirs, pl.ds(0, pivots)], target, sems, partner)
        sends.append((rhs[0].at[0], 1, sems))
        sends.append((rhs[0], nx - 1, sems))

    def rhs_halves():
        for level in range(1, LEVELS):
            send(
                rhs_ref.at[0, 0, theirs, pl.ds(level * pivots, pivots)],
                rhs[level].at[slot(level), core],
                rhs_sems(level, 3),
                partner,
            )
            sends.append((rhs[level].at[0], 1, rhs_sems(level, 3)))

    def give_inverse(level):
        loads[level].wait()
        cols = pl.ds(column_start(level), column_start(level + 1) - column_start(level))
        span = inverse_raw.at[core, :, cols]
        copy = pltpu.make_async_remote_copy(
            span, span, *weight_sems(level), device_id=partner, device_id_type=MESH
        )
        copy.start()
        return copy

    def give_update(level):
        if not level:
            loads[LEVELS].wait()
        cols = pl.ds(update_start(level), update_start(level + 1) - update_start(level))
        span = update_raw.at[core, :, cols]
        copy = pltpu.make_async_remote_copy(
            span, span, *weight_sems(LEVELS + level), device_id=partner, device_id_type=MESH
        )
        copy.start()
        return copy

    list_copies = [list_copy(level) for level in range(LEVELS - 1)]
    rhs_base()
    for copy in list_copies:
        copy.start()
    rhs_halves()
    given, given_update = {}, {}
    given[0] = give_inverse(0)
    given_update[0] = give_update(0)
    given[1] = give_inverse(1)
    given_update[1] = give_update(1)
    pivot_coefficients()
    coefficient_copy = pltpu.make_async_remote_copy(
        coefficients.at[core],
        coefficients.at[core],
        *weight_sems(2 * LEVELS),
        device_id=partner,
        device_id_type=MESH,
    )
    coefficient_copy.start()
    given[2] = give_inverse(2)
    given_update[2] = give_update(2)
    given[3] = give_inverse(3)

    def prepare(level):
        given[level].wait_recv()
        for block in range(column_start(level) // BLOCK, column_start(level + 1) // BLOCK):
            for parity in range(2):
                high, low = split(inverse_raw[parity, :, block * BLOCK : (block + 1) * BLOCK])
                start = parity * 2 * pivots
                inverse_split[block, start : start + pivots] = high
                inverse_split[block, start + pivots : start + 2 * pivots] = low

    def prepare_update(level):
        given_update[level].wait_recv()
        cols = slice(update_start(level), update_start(level + 1))
        for parity in range(2):
            high, low = split(update_raw[parity, :, cols])
            start = parity * 2 * pivots
            update_split[start : start + pivots, cols] = high
            update_split[start + pivots : start + 2 * pivots, cols] = low

    def fetch_lists(levels, own):
        for level in levels:
            list_copies[level].wait()
        lists = [(targets_ref, 0)] if own else []
        lists += [(targets_far.at[level], level + 1) for level in levels]
        copies = [
            pltpu.make_async_copy(source, targets_smem.at[index], load_sem.at[LEVELS + 1 + index])
            for source, index in lists
        ]
        for copy in copies:
            copy.start()
        for copy in copies:
            copy.wait()

    def half_ready(level):
        wait_recv(rhs[level].at[0], 1, rhs_sems(level, 3))

    def base_ready():
        wait_recv(rhs[0].reshape(nx * 2, half, pivots), 2 * nx - 1, rhs_sems(0, 0))

    def one_across():
        half_ready(1)

        @on(0)
        def _():
            each = rhs[1].at[rank(1)]
            send(each, each, rhs_sems(1, 0), peer(1, 2))

    def one_beside():
        def body(index):
            if index:
                wait_recv(rhs[1], index, rhs_sems(1, 0))
            for back in range(index + 1):
                each = rhs[1].at[rank(1) - 2 * back]
                send(each, each, rhs_sems(1, 1), peer(1, 1))

        for_column(body)

    def one_ready():
        for_column(lambda index: wait_recv(rhs[1], index + 1, rhs_sems(1, 1)))

    def pair_start():
        return lax.rem(lax.div(leaf, 2), 2) * (2 * nx)

    def two_beside():
        half_ready(2)
        each = rhs[2].at[slot(2)]
        send(each, each, rhs_sems(2, 1), peer(2, 1))
        sends.append((rhs[2], 1, rhs_sems(2, 1)))

    def two_across():
        wait_recv(rhs[2], 1, rhs_sems(2, 1))

        @on(0)
        def _():
            span = rhs[2].at[pl.ds(pair_start(), 2)]
            send(span, span, rhs_sems(2, 0), peer(2, 4))

    def two_deep():
        def body(index):
            if index:
                wait_recv(rhs[2], 2 * index, rhs_sems(2, 0))
            span = rhs[2].at[pl.ds(pair_start(), 2 * (index + 1))]
            send(span, span, rhs_sems(2, 2), peer(2, 2))

        for_column(body)

    def two_ready():
        for_column(lambda index: wait_recv(rhs[2], 2 * (index + 1), rhs_sems(2, 2)))

    def top_run(slot_row, slot_column):
        return rhs[TOP].at[pl.ds((slot_row * nx + slot_column) * DEPTH, DEPTH)]

    def top_deep():
        half_ready(TOP)
        each = rhs[TOP].at[slot(TOP)]
        for deep in range(DEPTH - 1, 0, -1):
            send(each, each, rhs_sems(TOP, 0), peer(TOP, 2 * deep))
        sends.append((rhs[TOP], DEPTH - 1, rhs_sems(TOP, 0)))

    def top_beside():
        run = top_run(row, column)
        send(run, run, rhs_sems(TOP, 2), peer(TOP, 1))

    def top_first():
        wait_recv(rhs[TOP], DEPTH - 1, rhs_sems(TOP, 0))

        @pl.when(core == 1)
        def _():
            top_beside()

        @on(0, 0)
        def _():
            run = top_run(row, 0)
            send(run, run, rhs_sems(TOP, 1), peer(TOP, 1 << TOP))

        sends.append((rhs[TOP], DEPTH, rhs_sems(TOP, 2)))

    def top_second():
        @pl.when(core == 0)
        def _():
            top_beside()

        @on(0, 1)
        def _():
            wait_recv(rhs[TOP], DEPTH, rhs_sems(TOP, 2))
            for each in range(2):
                run = top_run(each, 0)
                send(run, run, rhs_sems(TOP, 1), peer(TOP, 1 << TOP))

        @on(1, 0)
        def _():
            wait_recv(rhs[TOP], DEPTH, rhs_sems(TOP, 1))
            run = top_run(row, 0)
            send(run, run, rhs_sems(TOP, 2), peer(TOP, 1))

    def top_ready():
        @on(0, 0)
        def _():
            wait_recv(rhs[TOP], DEPTH, rhs_sems(TOP, 2))

        @on(1, 0)
        def _():
            wait_recv(rhs[TOP], 2 * DEPTH, rhs_sems(TOP, 2))

        @on(1, 1)
        def _():
            wait_recv(rhs[TOP], DEPTH, rhs_sems(TOP, 2))
            wait_recv(rhs[TOP], 2 * DEPTH, rhs_sems(TOP, 1))

    def rhs_drain():
        def body(index):
            if not index:
                wait_send(rhs[1], 1, rhs_sems(1, 0))
                wait_send(rhs[2], 2, rhs_sems(2, 0))
            wait_send(rhs[1], index + 1, rhs_sems(1, 1))
            wait_send(rhs[2], 2 * (index + 1), rhs_sems(2, 2))

        for_column(body)

        @on(0, 0)
        def _():
            wait_send(rhs[TOP], DEPTH, rhs_sems(TOP, 1))

        @on(0, 1)
        def _():
            wait_send(rhs[TOP], 2 * DEPTH, rhs_sems(TOP, 1))

        @on(1, 0)
        def _():
            wait_send(rhs[TOP], DEPTH, rhs_sems(TOP, 2))

    def group_of(key):
        return key[1] + (1 if key[0] == "up" else 0), key[1] + (0 if key[0] == "up" else 1)

    def key_sems(kind, key):
        index = keys.index(key)
        if kind == "gather":
            return gather_send.at[index], gather_recv.at[index]
        return scatter_send.at[index], scatter_recv.at[index]

    def gather_start(key, total):
        level, _ = group_of(key)
        buffer, sems = gathered[key], key_sems("gather", key)
        buffer[rank(level)] = total
        for mask in far_first(chips(level)):
            each = buffer.at[rank(level)]
            send(each, each, sems, peer(level, mask))
        sends.append((buffer, chips(level) - 1, sems))

    def gather_finish(key):
        level, _ = group_of(key)
        wait_recv(gathered[key], chips(level) - 1, key_sems("gather", key))

    def scatter_start(key):
        _, level = group_of(key)
        sems = key_sems("scatter", key)
        for mask in far_first(chips(level)):
            send(
                part[key].at[flip(rank(level), mask)],
                landed[key].at[mask - 1],
                sems,
                peer(level, mask),
            )
        sends.append((part[key], chips(level) - 1, sems))

    def scatter_finish(key):
        _, level = group_of(key)
        wait_recv(landed[key], chips(level) - 1, key_sems("scatter", key))
        total = part[key][rank(level)]
        for place in range(chips(level) - 1):
            total = total + landed[key][place]
        return total

    def chosen_columns(level, child, index):
        place = update_start(level) // BLOCK + index
        upper = lax.rem(lax.div(leaf, 1 << level), 2)
        near, far = targets_smem[0, 0, place], targets_smem[level + 1, 0, place]
        block = near + (far - near) * (upper + child - 2 * upper * child)
        return inverse_split[column_start(level + 1) // BLOCK + block]

    def known_part(level):
        product = None
        for index in range(chips(level)):
            values = jnp.concatenate([rhs[level][index, parity] for parity in range(2)], 1)
            matrix = jnp.concatenate(
                [inverse_split[block] for block in slot_blocks(level, index)], 1
            )
            term = along_columns(rows_of(values), matrix)
            product = term if product is None else product + term
        return product

    def sent_up(solved, level):
        start, blocks = update_start(level), block_count(level)
        partial = across(square_of(solved), update_split[:, start : start + blocks * BLOCK])
        for block in range(blocks):
            part["up", level][block] = partial[:, block * BLOCK : (block + 1) * BLOCK]
        scatter_start(("up", level))

    def less_children(product, level):
        below = level - 1
        buffer = gathered["up", below]
        for child in range(2):
            for index in range(0, block_count(below), 2):
                pair = (index, index + 1)
                values = [buffer[slot_at(below, child, i)] for i in pair]
                matrices = [chosen_columns(below, child, i) for i in pair]
                product = product - along_columns(
                    rows_of(jnp.concatenate(values, 1)), jnp.concatenate(matrices, 1)
                )
        return product

    def sent_down(square, level):
        key = ("down", level - 1)
        for child in range(2):
            for index in range(0, block_count(level - 1), 2):
                pair = (index, index + 1)
                matrix = jnp.concatenate(
                    [chosen_columns(level - 1, child, i) for i in pair], 1
                )
                partial = across(square, matrix)
                for j, i in enumerate(pair):
                    part[key][slot_at(level - 1, child, i)] = partial[
                        :, j * BLOCK : (j + 1) * BLOCK
                    ]
        scatter_start(key)

    def with_parent(level):
        buffer = gathered["down", level]
        product = None
        for index in range(0, block_count(level), 2):
            values = jnp.concatenate([buffer[index], buffer[index + 1]], 1)
            start = update_start(level) + index * BLOCK
            term = along_columns(rows_of(values), update_split[:, start : start + 2 * BLOCK])
            product = term if product is None else product + term
        return weighted[level] - fold(product)

    def out_sems(level, phase):
        return out_send.at[level, phase], out_recv.at[level, phase]

    def made_out(square, level):
        for index in range(chips(level)):
            matrix = jnp.concatenate(
                [inverse_split[block] for block in slot_blocks(level, index)], 1
            )
            partial = across(square, matrix)
            for parity in range(2):
                out_part[level][index, parity] = partial[
                    :, parity * pivots : (parity + 1) * pivots
                ]

    def plain_out_start(level):
        sems = out_sems(level, 0)

        def one(mask):
            send(
                out_part[level].at[flip(rank(level), mask)],
                out_landed[level].at[mask - 1],
                sems,
                peer(level, mask),
            )

        @on(1)
        def _():
            for mask in far_first(chips(level)):
                if mask >> level:
                    one(mask)

        for mask in far_first(1 << level):
            one(mask)

    def plain_out_finish(level):
        def body(index):
            fewer = chips(level) if index == 0 else 1 << level
            if fewer > 1:
                wait_recv(out_landed[level], fewer - 1, out_sems(level, 0))

        for_column(body)
        total = out_part[level][rank(level)]
        for place in range(chips(level) - 1):
            total = total + out_landed[level][place]
        return total

    def plain_out_drain(level):
        def body(index):
            fewer = chips(level) if index else 1 << level
            if fewer > 1:
                wait_send(out_landed[level], fewer - 1, out_sems(level, 0))

        for_column(body)

    def out_add(level, start, place, count):
        span = pl.ds(start, count)
        out_part[level][span] = out_part[level][span] + out_landed[level][place : place + count]

    def middle_first():
        other = (1 - lax.rem(lax.div(leaf, 2), 2)) * (2 * nx)

        def body(index):
            each = 2 * (index + 1)
            send(
                out_part[2].at[pl.ds(other, each)],
                out_landed[2].at[pl.ds(0, each)],
                out_sems(2, 0),
                peer(2, 2),
            )

        for_column(body)

    def middle_second():
        here = pair_start() + row
        beside = pair_start() + 1 - row

        def body(index):
            each = 2 * (index + 1)
            wait_recv(out_landed[2], each, out_sems(2, 0))
            out_add(2, pair_start(), 0, each)
            if index:
                for place, source, mask in ((1, beside, 5), (0, here, 4)):
                    send(
                        out_part[2].at[source],
                        out_landed[2].at[2 * nx + place],
                        out_sems(2, 1),
                        peer(2, mask),
                    )
            send(
                out_part[2].at[beside + 2 * index],
                out_landed[2].at[2 * nx + 2],
                out_sems(2, 1),
                peer(2, 1),
            )

        for_column(body)

    def middle_finish():
        def body(index):
            wait_recv(out_landed[2], 1 if index else nx + 1, out_sems(2, 1))

        for_column(body)
        total = out_part[2][slot(2)]
        for place in range(3):
            total = total + out_landed[2][2 * nx + place]
        return total

    def middle_drain():
        def body(index):
            wait_send(out_landed[2], 2 * (index + 1), out_sems(2, 0))
            wait_send(out_landed[2], nx + 1 if index else 1, out_sems(2, 1))

        for_column(body)

    def final_index(slot_row, slot_column):
        return (slot_row * nx + slot_column) * DEPTH

    def final_run(slot_row, slot_column, count=1):
        return out_part[TOP].at[pl.ds(final_index(slot_row, slot_column), count * DEPTH)]

    def final_first():
        for index in range(nx):

            @on(index, 0)
            def _():
                send(
                    final_run(1 - row, 0, index + 1),
                    out_landed[TOP].at[pl.ds(0, (index + 1) * DEPTH)],
                    out_sems(TOP, 0),
                    peer(TOP, 1),
                )

        @on(1, 1)
        def _():
            for each in range(2):
                send(
                    final_run(each, 0),
                    out_landed[TOP].at[pl.ds(each * DEPTH, DEPTH)],
                    out_sems(TOP, 0),
                    peer(TOP, 1 << TOP),
                )

    def final_second():
        there = out_landed[TOP].at[pl.ds(2 * DEPTH, DEPTH)]
        for index in range(nx):

            @on(index, 0)
            def _():
                wait_recv(out_landed[TOP], (index + 1) * DEPTH, out_sems(TOP, 0))
                out_add(TOP, final_index(row, 0), 0, (index + 1) * DEPTH)

        @on(1, 0)
        def _():
            send(final_run(row, 0), there, out_sems(TOP, 1), peer(TOP, 1 << TOP))

        @on(0, 1)
        def _():
            wait_recv(out_landed[TOP], 2 * DEPTH, out_sems(TOP, 0))
            for each in range(2):
                out_add(TOP, final_index(each, 0), each * DEPTH, DEPTH)

        @pl.when(core == 1)
        def _():
            send(final_run(1 - row, column), there, out_sems(TOP, 1), peer(TOP, 1))

    def final_third():
        @pl.when((core == 1) | (column == 0))
        def _():
            wait_recv(out_landed[TOP], DEPTH, out_sems(TOP, 1))
            out_add(TOP, final_index(row, column), 2 * DEPTH, DEPTH)

        deep = lax.rem(lax.div(leaf, 2), DEPTH)
        for mask in range(DEPTH - 1, 0, -1):
            send(
                out_part[TOP].at[final_index(row, column) + flip(deep, mask)],
                out_landed[TOP].at[3 * DEPTH + mask - 1],
                out_sems(TOP, 2),
                peer(TOP, 2 * mask),
            )
        sends.append((out_landed[TOP], DEPTH - 1, out_sems(TOP, 2)))

    def final_finish():
        wait_recv(out_landed[TOP], DEPTH - 1, out_sems(TOP, 2))
        total = out_part[TOP][slot(TOP)]
        for place in range(DEPTH - 1):
            total = total + out_landed[TOP][3 * DEPTH + place]
        return total

    def final_drain():
        for index in range(nx):

            @on(index, 0)
            def _():
                wait_send(out_landed[TOP], (index + 1) * DEPTH, out_sems(TOP, 0))

        @on(1, 1)
        def _():
            wait_send(out_landed[TOP], 2 * DEPTH, out_sems(TOP, 0))

        @pl.when((core == 1) | (column == 1))
        def _():
            wait_send(out_landed[TOP], DEPTH, out_sems(TOP, 1))

    def swap_sems(level):
        return swap_send.at[level], swap_recv.at[level]

    def result_start(level, total):
        result_near[level] = total
        send(
            result_near.at[level, 1 - core], result_far.at[level], swap_sems(level), partner
        )
        sends.append((result_far, 1, swap_sems(level)))
        out_ref[0, 0, mine, level_cols(level)] = result_near[level, core]

    def result_finish(level):
        wait_recv(result_far, 1, swap_sems(level))
        out_ref[0, 0, theirs, level_cols(level)] = result_far[level]

    group, wide = chips(1), nx
    corner = rank(1)

    def side(index):
        return side_send.at[index], side_recv.at[index]

    def turned(level):
        cols = slice(update_start(level), update_start(level + 1))
        straight, crossed = [], []
        for parity in range(2):
            high, low = split(update_raw[parity, :, cols].T)
            straight += [high, low]
            crossed += [low, high]
        return jnp.concatenate(
            [jnp.concatenate(straight, 1), jnp.concatenate(crossed, 1)], 0
        )

    def cross_start():
        picks = [chosen_columns(0, child, core) for child in range(2)]
        product = across(turned(1), jnp.concatenate(picks, 1))
        for block in range(group):
            for i in range(wide):
                cross_part[block, i] = product[
                    block * pivots : (block + 1) * pivots, i * pivots : (i + 1) * pivots
                ]
        for mask in far_first(group):
            send(
                cross_part.at[flip(corner, mask)],
                cross_landed.at[mask - 1],
                side(1),
                peer(1, mask),
            )
        sends.append((cross_landed, group - 1, side(1)))

    def cross_share():
        wait_recv(cross_landed, group - 1, side(1))
        total = cross_part[corner]
        for place in range(group - 1):
            total = total + cross_landed[place]
        span = cross_row.at[pl.ds(core * wide, wide)]
        cross_row[pl.ds(core * wide, wide)] = total
        send(span, span, side(2), partner)
        sends.append((cross_row, wide, side(2)))

    def cross_rows():
        wait_recv(cross_row, wide, side(2))
        for block in range(group):
            cols = slice(block * pivots, (block + 1) * pivots)
            high, low = split(cross_row[block])
            cross_row_split[:pivots, cols] = high
            cross_row_split[pivots:, cols] = low

    def cross_turn():
        for mask in far_first(group):
            send(cross_row.at[flip(corner, mask)], cross_col.at[corner], side(3), peer(1, mask))
        sends.append((cross_row, group - 1, side(3)))
        cross_col[corner] = cross_row[corner]

    def cross_columns():
        wait_recv(cross_col, group - 1, side(3))
        for block in range(group):
            high, low = split(cross_col[block])
            cross_col_split[block, :pivots] = high
            cross_col_split[block, pivots:] = low

    def low_start():
        left = turned(0)
        for target in range(nx):
            product = across(left, inverse_split[target * 2 + core])
            for i in range(nx):
                low_part[target, i] = product[i * pivots : (i + 1) * pivots]

    def low_spread():
        @on(1)
        def _():
            send(low_part.at[0], low_landed, side(4), peer(0, 1))

    def low_share():
        @on(0)
        def _():
            wait_recv(low_landed, nx, side(4))
            low_part[0] = low_part[0] + low_landed[...]

        low_sum[core] = low_part[column]
        send(low_sum.at[core], low_sum.at[core], side(5), partner)
        sends.append((low_landed, nx, side(5)))

    def low_finish():
        wait_recv(low_landed, nx, side(5))
        for i in range(nx):
            for parity in range(2):
                cols = slice(parity * pivots, (parity + 1) * pivots)
                high, low = split(low_sum[parity, i])
                low_split[i, :pivots, cols] = high
                low_split[i, pivots:, cols] = low

    def low_drain():
        @on(1)
        def _():
            wait_send(low_landed, nx, side(4))

    weighted = []
    one_across()
    two_beside()
    top_deep()
    prepare(0)
    prepare_update(0)
    base_ready()
    solved = fold(known_part(0))
    sent_up(solved, 0)
    one_beside()
    fetch_lists([0], True)
    two_across()
    prepare(1)
    prepare_update(1)
    cross_start()
    total = scatter_finish(("up", 0))
    gather_start(("up", 0), total)
    one_ready()
    known = known_part(1)
    sent_up(fold(known), 1)
    top_first()
    two_deep()
    fetch_lists(list(range(1, LEVELS - 1)), False)
    prepare(2)
    prepare_update(2)
    coefficient_copy.wait_recv()
    weighted.append(pivot_solve(solved, 0))
    low_start()
    gather_finish(("up", 0))
    cross_share()
    total = scatter_finish(("up", 1))
    cross_rows()
    values = [gathered["up", 0][block] for block in range(group)]
    total = total - fold(
        along_columns(rows_of(jnp.concatenate(values, 1)), cross_row_split[...])
    )
    gather_start(("up", 1), total)
    low_spread()
    solved = fold(less_children(known, 1))
    weighted.append(pivot_solve(solved, 1))
    top_second()
    two_ready()
    product = known_part(2)
    prepare(3)
    gather_finish(("up", 1))
    solved = fold(less_children(product, 2))
    sent_up(solved, 2)
    weighted.append(pivot_solve(solved, 2))
    low_share()
    total = scatter_finish(("up", 2))
    gather_start(("up", 2), total)
    cross_turn()
    sent_down(square_of(weighted[1]), 1)
    top_ready()
    product = known_part(3)
    low_finish()
    gather_finish(("up", 2))
    solved = fold(less_children(product, 3))
    weighted.append(pivot_solve(solved, 3))

    square = square_of(weighted[3])
    sent_down(square, 3)
    made_out(square, 3)
    final_first()
    made_out(square_of(weighted[0]), 0)
    plain_out_start(0)
    cross_columns()
    small = scatter_finish(("down", 0))
    total = scatter_finish(("down", 2))
    gather_start(("down", 2), total)
    final_second()
    gather_finish(("down", 2))
    square = square_of(with_parent(2))
    sent_down(square, 2)
    made_out(square, 2)
    middle_first()
    final_third()
    base = plain_out_finish(0)
    total = scatter_finish(("down", 1))
    gather_start(("down", 1), total)
    middle_second()
    gather_finish(("down", 1))
    made_out(square_of(with_parent(1)), 1)
    plain_out_start(1)
    for block in range(group):
        small = small - across(square_of(gathered["down", 1][block]), cross_col_split[block])
    gather_start(("down", 0), small)
    result_start(3, final_finish())
    gather_finish(("down", 0))
    base = jnp.concatenate([base[0], base[1]], 1)
    for block in range(block_count(0)):
        base = base - across(square_of(gathered["down", 0][block]), low_split[block])
    result_start(0, jnp.stack([base[:, :pivots], base[:, pivots:]]))
    result_start(2, middle_finish())
    result_start(1, plain_out_finish(1))
    for level in (3, 0, 2, 1):
        result_finish(level)
    for item in sends:
        wait_send(*item)
    rhs_drain()
    for level in range(2):
        plain_out_drain(level)
    middle_drain()
    final_drain()
    low_drain()
    for copy in [*given.values(), *given_update.values(), coefficient_copy]:
        copy.wait_send()


def per_device(*arguments):
    right_side, factor_inverse, update_panel = arguments[:3]
    pivots = factor_inverse.shape[2]
    half = right_side.shape[2] // 2
    nx = lax.axis_size("front") // 2
    keys = [(kind, level) for kind in ("up", "down") for level in range(LEVELS - 1)]
    targets = (8, BLOCK)
    group, wide = nx << 1, nx
    blocks = factor_inverse.shape[3] // BLOCK
    buffers = []
    for _ in range(2):
        buffers += [pltpu.VMEM((nx << level, 2, half, pivots), F32) for level in range(LEVELS)]
    buffers += [pltpu.VMEM((nx << level, 2, half, pivots), F32) for level in range(LEVELS)]
    for kind, level in keys:
        wider, narrower = (nx << level + 1, nx << level)
        first, second = (wider, narrower) if kind == "up" else (narrower, wider)
        buffers += [pltpu.VMEM((count, half, BLOCK), F32) for count in (first, second, second)]
    vmem = pl.BlockSpec(memory_space=pltpu.VMEM)
    hbm = pl.BlockSpec(memory_space=pl.ANY)
    dma = pltpu.SemaphoreType.DMA
    square = (pivots, pivots)
    return pl.pallas_call(
        functools.partial(kernel, nx, pivots, keys),
        out_shape=pltpu.VMEM(right_side.shape, F32),
        in_specs=[vmem, hbm, hbm, vmem, vmem, vmem, vmem],
        out_specs=vmem,
        scratch_shapes=[
            pltpu.VMEM((2,) + factor_inverse.shape[2:], F32),
            pltpu.VMEM((2,) + update_panel.shape[2:], F32),
            pltpu.VMEM((blocks, 4 * pivots, BLOCK), BF16),
            pltpu.VMEM((4 * pivots, update_panel.shape[3]), BF16),
            pltpu.VMEM((2, 2, 8, LEVELS * pivots), F32),
            pltpu.VMEM(targets, jnp.int32),
            pltpu.VMEM((LEVELS - 1,) + targets, jnp.int32),
            pltpu.SMEM((LEVELS,) + targets, jnp.int32),
            pltpu.VMEM((LEVELS, 2, half, pivots), F32),
            pltpu.VMEM((LEVELS, half, pivots), F32),
            pltpu.VMEM((group, wide) + square, F32),
            pltpu.VMEM((group - 1, wide) + square, F32),
            pltpu.VMEM((group,) + square, F32),
            pltpu.VMEM((group,) + square, F32),
            pltpu.VMEM((2 * pivots, group * pivots), BF16),
            pltpu.VMEM((group, 2 * pivots, pivots), BF16),
            pltpu.VMEM((nx, nx) + square, F32),
            pltpu.VMEM((nx,) + square, F32),
            pltpu.VMEM((2, nx) + square, F32),
            pltpu.VMEM((nx, 2 * pivots, 2 * pivots), BF16),
            dma((2 * LEVELS + 1,)),
            dma((LEVELS - 1,)),
            dma((LEVELS - 1,)),
            dma((2 * LEVELS + 1,)),
            dma((2 * LEVELS + 1,)),
            dma((6,)),
            dma((6,)),
            dma((LEVELS, 4)),
            dma((LEVELS, 4)),
            dma((LEVELS, 3)),
            dma((LEVELS, 3)),
            dma((LEVELS,)),
            dma((LEVELS,)),
            dma((len(keys),)),
            dma((len(keys),)),
            dma((len(keys),)),
            dma((len(keys),)),
            *buffers,
        ],
        compiler_params=pltpu.CompilerParams(collective_id=0, has_side_effects=True),
    )(*arguments)


def solution(mesh):
    in_specs = (
        P("leaf", "front", None, None),
        P("leaf", "front", None, None),
        P("leaf", "front", None, None),
        P("leaf", None),
        P("leaf", "front", None),
        P("leaf", "front", None),
        P("leaf", "front", None),
    )
    out_specs = P("leaf", "front", None, None)
    return jax.shard_map(
        per_device, mesh=mesh, in_specs=in_specs, out_specs=out_specs, check_vma=False
    )
```
